128 devices in a mesh: blk: 8 (over x, y_lo), uly: 2 (over core), dp: 8 (over z, y_hi).
Axes of the slice: x: 4, y: 4 (y_hi: 2, y_lo: 2; y = y_hi * 2 + y_lo), z: 4, core: 2. Of those that a mesh axis runs over, the one named last changes fastest.
Arguments:
- short_tokens: bfloat16 [64, 1024, 4096], P(('blk', 'dp'), 'uly'), may hold values from -150 to 150, as said below
- short_segments: int32 [64, 1024], P(('blk', 'dp')), may hold values from 0 to 3, never falling along the last dimension, each value on 1 to 512 neighbouring positions
- long_tokens: bfloat16 [8, 3072, 4096], P('dp', 'blk'), may hold values from -150 to 150, as said below
- long_lengths: int32 [8], P('dp'), may hold values from 768 to 3072
- w_query: bfloat16 [4096, 2048], P(('blk', 'dp'), 'uly'), may hold values from -0.09375 to 0.09375
- w_key: bfloat16 [4096, 512], P(('blk', 'dp'), 'uly'), may hold values from -0.09375 to 0.09375
- w_value: bfloat16 [4096, 512], P(('blk', 'dp'), 'uly'), may hold values from -0.09375 to 0.09375
Outputs:
- short_out: bfloat16 [64, 1024, 2048], P(('blk', 'dp'), 'uly')
- long_out: bfloat16 [8, 3072, 2048], P('dp', 'blk', 'uly')
The draws below stay inside these ranges and needn't reach their ends.
Inputs may be any that keep to these rules, and one draw needn't show every extreme that they name: `short_tokens`: activations of the short bucket. `long_tokens`: activations of the long bucket; rows at or after a sequence's length are padding. `short_segments`: document numbers never fall along a sequence. `long_lengths`: a long sequence occupies positions 0 to its length - 1 of its 3072 slots.
All inputs are finite; a program needn't handle non-finite values.
Results may differ from the reference program's by a relative error of at most 0.012.
The reference program's roundings to bfloat16 on the way count: a program that leaves them out, or rounds other values in their place, can miss the bound.
Values may be sent and summed in bfloat16 or wider, within the bound.
A program may use at most 128 MiB of HBM per device.

```python
import math
import jax
import jax.numpy as jnp
import numpy as np
from jax import lax

D = 4096
HQ = 16
HK = 4
HD = 128
LS = 1024
NS = 64
NL = 8
LL = 3072


def token_rows(key, shape):
    base = jnp.clip(jax.random.normal(key, shape, jnp.float32), -6.0, 6.0)
    return base.astype(jnp.bfloat16)


def draw_short_tokens(key, part):
    return token_rows(jax.random.fold_in(key, 101), (NS, LS, D))


def draw_long_tokens(key, part):
    return token_rows(jax.random.fold_in(key, 202), (NL, LL, D))


def plant(values, stream_key, low, largest):
    place = [jax.random.randint(jax.random.fold_in(stream_key, axis), (), 0, length) for axis, length in enumerate(values.shape)]
    longest = values.shape.index(max(values.shape))
    neighbour = place[:longest] + [(place[longest] + 1) % values.shape[longest]] + place[longest + 1:]
    return values.at[tuple(place)].set(low).at[tuple(neighbour)].set(largest)


def levels(rng, dims, shards, least, top_value):
    def one(dim, blocks):
        heights = jax.random.uniform(jax.random.fold_in(jax.random.fold_in(rng, 6), dim), (blocks,), jnp.float32, least / len(shards), top_value / len(shards))
        return jnp.repeat(jnp.exp(heights), dims[dim] // blocks).reshape((-1,) + (1,) * (len(dims) - dim - 1))

    loudness = one(*shards[0])
    for cut in shards[1:]:
        loudness = loudness * one(*cut)
    return loudness


def length_profile(number_of, total, most, lean):
    weights = [(1 << 20) // math.isqrt(grade ** lean) + 1 for grade in range(2, number_of + 1)]
    spare, counts = total - most - (number_of - 1), [1] * (number_of - 1)
    while spare > 0:
        movable = [i for i in range(number_of - 1) if counts[i] < most]
        whole, remaining = sum([weights[i] for i in movable]), spare
        for i in movable:
            extra = min(most - counts[i], max(1, remaining * weights[i] // whole), spare)
            counts[i] = counts[i] + extra
            spare = spare - extra
    return np.array([most] + counts)


def uneven(own_key, number_of, total, most, lean):
    if number_of == 2:
        one = jax.random.randint(own_key, (), max(1, total - most), min(most, total - 1) + 1)
        return jnp.stack([one, total - one])
    lengths = jnp.asarray(length_profile(number_of, total, most, lean), jnp.int32)
    twos = (number_of - 1) // 2
    donor, receiver = lengths[1:1 + 2 * twos:2], lengths[2:2 + 2 * twos:2]
    room = jnp.minimum(donor - 1, most - receiver)
    shifted = jax.random.randint(jax.random.fold_in(own_key, 1), (twos,), 0, 1 << 20) % (room + 1)
    lengths = lengths.at[1:1 + 2 * twos:2].set(donor - shifted).at[2:2 + 2 * twos:2].set(receiver + shifted)
    return lengths[jax.random.permutation(jax.random.fold_in(own_key, 2), number_of)]


def gaussian(own_key, extent, width, bound, split=(), kind=jnp.bfloat16):
    factor_of = levels(own_key, extent, split, -0.22, 0.18) if split else 1.0
    drawn = jax.random.normal(own_key, extent, jnp.float32) * width * factor_of
    return jnp.minimum(jnp.maximum(drawn, -bound), bound).astype(kind)


def setup_inputs(seed: int = 0) -> dict:
    keys = jax.random.split(jax.random.key(seed), 8)
    short_tokens = draw_short_tokens(jax.random.fold_in(keys[7], 71), 0)
    short_segments = jax.vmap(lambda own: jnp.searchsorted(jnp.cumsum(uneven(own, 4, LS, LS // 2, 1)), jnp.arange(LS), side="right"))(jax.random.split(keys[1], NS)).reshape((NS, LS)).astype(jnp.int32)
    long_tokens = draw_long_tokens(jax.random.fold_in(keys[7], 71), 0)
    long_lengths = plant(jax.random.randint(keys[3], (NL,), LL // 4, LL + 1), jax.random.fold_in(keys[3], 1), LL // 4, LL).astype(jnp.int32)
    w_query = gaussian(keys[4], (D, HQ * HD), D ** -0.5, 0.09375, ((0, 64), (1, 2)))
    w_key = gaussian(keys[5], (D, HK * HD), D ** -0.5, 0.09375, ((0, 64), (1, 2)))
    w_value = gaussian(keys[6], (D, HK * HD), D ** -0.5, 0.09375, ((0, 64), (1, 2)))
    return {"short_tokens": short_tokens, "short_segments": short_segments, "long_tokens": long_tokens, "long_lengths": long_lengths, "w_query": w_query, "w_key": w_key, "w_value": w_value}


masked_score = -1e+30

def rounded_wide(array):
    return lax.optimization_barrier(array.astype(jnp.bfloat16)).astype(jnp.float32)

def project(rows, weight):
    return jnp.dot(rows, weight, preferred_element_type=jnp.float32)

def attention(queries, key_rows, value_rows, visible_rows):
    seq_len = key_rows.shape[0]
    block_rows = min(512, seq_len)
    group_size = HQ // HK
    key_heads = key_rows.reshape(seq_len, HK, HD)
    value_heads = value_rows.reshape(seq_len, HK, HD)
    outputs = []
    for block_index in range(seq_len // block_rows):
        first_row = block_index * block_rows
        query_heads = queries[first_row:first_row + block_rows].reshape(block_rows, HK, group_size, HD)
        visible = visible_rows(first_row, block_rows)
        scores = jnp.einsum('bhgd,khd->hgbk', query_heads, key_heads) * (1.0 / math.sqrt(HD))
        scores = jnp.where(visible, scores, masked_score)
        row_max = lax.optimization_barrier(jnp.max(scores, axis=-1, keepdims=True))
        exponentials = jnp.where(visible, jnp.exp(scores - row_max), 0.0)
        totals = lax.optimization_barrier(jnp.sum(exponentials, axis=-1))
        mixed = jnp.einsum('hgbk,khd->hgbd', rounded_wide(exponentials), value_heads)
        mixed = mixed / totals[..., None]
        outputs.append(jnp.transpose(mixed, (2, 0, 1, 3)).reshape(block_rows, HQ * HD))
    return jnp.concatenate(outputs, axis=0)

def reference(short_tokens, short_segments, long_tokens, long_lengths, w_query, w_key, w_value):

    def one_short(inputs):
        rows, segments = inputs
        queries = rounded_wide(project(rows, w_query))
        key_rows = rounded_wide(project(rows, w_key))
        value_rows = rounded_wide(project(rows, w_value))
        positions = jnp.arange(rows.shape[0], dtype=jnp.int32)

        def visible_rows(first_row, block_rows):
            query_pos = positions[first_row:first_row + block_rows]
            query_seg = segments[first_row:first_row + block_rows]
            return (positions[None, :] <= query_pos[:, None]) & (segments[None, :] == query_seg[:, None])
        mixed = attention(queries, key_rows, value_rows, visible_rows)
        return mixed.astype(jnp.bfloat16)

    def one_long(inputs):
        rows, length = inputs
        queries = rounded_wide(project(rows, w_query))
        key_rows = rounded_wide(project(rows, w_key))
        value_rows = rounded_wide(project(rows, w_value))
        positions = jnp.arange(rows.shape[0], dtype=jnp.int32)

        def visible_rows(first_row, block_rows):
            query_pos = positions[first_row:first_row + block_rows]
            return (positions[None, :] <= query_pos[:, None]) & (positions[None, :] < length)
        mixed = attention(queries, key_rows, value_rows, visible_rows)
        mixed = jnp.where(positions[:, None] < length, mixed, 0.0)
        return mixed.astype(jnp.bfloat16)
    short_out = lax.map(one_short, (short_tokens, short_segments))
    long_out = lax.map(one_long, (long_tokens, long_lengths))
    return (short_out, long_out)
```

```python
import math

import jax
import jax.numpy as jnp
from jax import lax
from jax.experimental import pallas as pl
from jax.experimental.pallas import tpu as pltpu
from jax.sharding import PartitionSpec as P

MESH = pl.DeviceIdType.MESH
BF16 = jnp.bfloat16
F32 = jnp.float32
HD = 128
D = 4096
SEQ = 1024
HALF = 512
LONG = 384
ROWS = SEQ + LONG
GROUPS = 6
WIDTH = 256
HIDDEN = -1e30
SCALE = math.log2(math.e) / math.sqrt(HD)

PARTS = ((0, 32, "xyz"), (32, 16, "yzx"), (48, 16, "zxy"))

NT = (((1,), (1,)), ((), ()))


def kernel(
    xs_hbm, seg_ref, xl_hbm, len_ref, wq_hbm, wk_hbm, wv_hbm,
    so_hbm, lo_hbm,
    w, x, kb, vb, qb, kvl, sob, lob, bias_s, bias_l, q2, acc, mx, tot,
    send_sem, recv_sem, kv_send, kv_recv, x_sem, own_sem, out_send, out_recv, out_own,
):
    blk, core, dp = lax.axis_index("blk"), lax.axis_index("uly"), lax.axis_index("dp")
    cx, yl = blk // 2, blk % 2
    cz, yh = dp // 2, dp % 2
    cy = yh * 2 + yl
    here = {"x": cx, "y": cy, "z": cz}

    def device(dim, step):
        at = dict(here)
        at[dim] = (here[dim] + step + 4) % 4
        return (at["x"] * 2 + at["y"] % 2, core, at["z"] * 2 + at["y"] // 2)

    sibling = (blk, 1 - core, dp)

    own = [
        pltpu.make_async_copy(wk_hbm, w.at[0, cx, yl, cz, yh], own_sem.at[0]),
        pltpu.make_async_copy(wv_hbm, w.at[1, cx, yl, cz, yh], own_sem.at[1]),
    ]
    for g in range(4):
        own.append(
            pltpu.make_async_copy(
                wq_hbm.at[:, pl.ds(g * WIDTH, WIDTH)], w.at[2 + g, cx, yl, cz, yh], own_sem.at[2 + g]
            )
        )
    my_rows = pl.ds(pl.multiple_of(core * HALF, HALF), HALF)
    own_x = pltpu.make_async_copy(xs_hbm.at[0], x.at[my_rows], x_sem.at[0])
    own_l = pltpu.make_async_copy(xl_hbm.at[0], x.at[pl.ds(SEQ, LONG)], x_sem.at[1])
    for copy in own + [own_l, own_x]:
        copy.start()

    barrier = pltpu.get_barrier_semaphore()
    for dim in "xyz":
        for step in (1, -1):
            pl.semaphore_signal(barrier, inc=1, device_id=device(dim, step), device_id_type=MESH)
    pl.semaphore_signal(barrier, inc=1, device_id=sibling, device_id_type=MESH)
    pl.semaphore_wait(barrier, 7)

    peer_x = pltpu.make_async_remote_copy(
        src_ref=xs_hbm.at[0], dst_ref=x.at[my_rows], send_sem=x_sem.at[2], recv_sem=x_sem.at[3],
        device_id=sibling, device_id_type=MESH,
    )
    for copy in own:
        copy.wait()

    def block(groups, part, phase, position, half=None):
        first, count, order = PARTS[part]
        dim = order[phase]
        at = dict(here)
        at[dim] = position
        done = order[:phase]
        ix = slice(None) if "x" in done else at["x"]
        iz = slice(None) if "z" in done else at["z"]
        il = slice(None) if "y" in done else at["y"] % 2
        ih = slice(None) if "y" in done else at["y"] // 2
        columns = slice(None)
        if half is not None:
            if phase == 0:
                columns = pl.ds(half * 128, 128)
            elif order[0] == "x":
                ix = pl.ds(2 * half, 2)
            elif order[0] == "z":
                iz = pl.ds(2 * half, 2)
            else:
                il = half
        return w.at[groups, ix, il, iz, ih, pl.ds(first, count), columns]

    def hop(groups, stage, part, phase, slot):
        dim = PARTS[part][2][phase]
        step = 1 if slot % 2 == 0 else -1
        if slot < 2:
            ref = block(groups, part, phase, here[dim])
        else:
            ref = block(groups, part, phase, (here[dim] - step + 4) % 4, half=slot % 2)
        return pltpu.make_async_remote_copy(
            src_ref=ref, dst_ref=ref,
            send_sem=send_sem.at[stage, part, slot], recv_sem=recv_sem.at[stage, part, slot],
            device_id=device(dim, step), device_id_type=MESH,
        )

    sent = []

    def send(phase, g, second):
        groups = slice(None) if phase == 0 else g
        stage = 0 if phase == 0 else 1 + (phase - 1) * GROUPS + g
        for part in range(3):
            for slot in (2, 3) if second else (0, 1):
                copy = hop(groups, stage, part, phase, slot)
                copy.start()
                sent.append(copy)

    def arrive(phase, g, second):
        groups = slice(None) if phase == 0 else g
        stage = 0 if phase == 0 else 1 + (phase - 1) * GROUPS + g
        for part in range(3):
            for slot in (2, 3) if second else (0, 1):
                hop(groups, stage, part, phase, slot).wait_recv()

    def kv_copy(index, ref, dim, step):
        return pltpu.make_async_remote_copy(
            src_ref=ref, dst_ref=ref, send_sem=kv_send.at[index], recv_sem=kv_recv.at[index],
            device_id=device(dim, step) if dim == "x" else ((cx * 2 + 1 - yl), core, dp), device_id_type=MESH,
        )

    def kv_hops(index):
        left, right = (cx + 3) % 4, (cx + 1) % 4
        if index == 0:
            return kv_copy(0, kvl.at[cx, yl, pl.ds(0, 2)], "y", 0)
        if index in (1, 2):
            return kv_copy(index, kvl.at[cx, yl, pl.ds(2, 2)], "x", 1 if index == 1 else -1)
        if index in (3, 4):
            return kv_copy(index, kvl.at[cx, :, pl.ds(0, 2)], "x", 1 if index == 3 else -1)
        if index == 5:
            return kv_copy(5, kvl.at[left, yl, 2], "x", 1)
        if index == 6:
            return kv_copy(6, kvl.at[right, yl, 3], "x", -1)
        if index == 7:
            return kv_copy(7, kvl.at[left, 0, pl.ds(0, 2)], "x", 1)
        if index == 8:
            return kv_copy(8, kvl.at[right, 1, pl.ds(0, 2)], "x", -1)
        return kv_copy(9, kvl.at[:, yl, pl.ds(2, 2)], "y", 0)

    def kv_start(*indices):
        for index in indices:
            copy = kv_hops(index)
            copy.start()
            sent.append(copy)

    def kv_wait(*indices):
        for index in indices:
            kv_hops(index).wait_recv()

    def project(g, out):
        tile = 352

        @pl.loop(0, ROWS // tile)
        def _(i):
            rows = pl.ds(pl.multiple_of(i * tile, 32), tile)
            out[rows, :] = jnp.dot(
                x[rows, :], w[g].reshape(D, WIDTH), preferred_element_type=F32
            ).astype(BF16)

    def short_bias():
        @pl.loop(0, 8)
        def _(i):
            first = pl.multiple_of(i * 128, 128)
            own_seg = seg_ref[:, pl.ds(first, 128)].astype(F32)
            query_seg = jnp.transpose(jnp.broadcast_to(own_seg, (128, 128)))
            window = jnp.maximum(i // 2 - 2, 0) * 256
            for j in range(6):
                start = pl.multiple_of(window + j * 128, 128)
                key_seg = jnp.broadcast_to(seg_ref[:, pl.ds(start, 128)].astype(F32), (128, 128))
                query_pos = first + lax.broadcasted_iota(jnp.int32, (128, 128), 0)
                key_pos = start + lax.broadcasted_iota(jnp.int32, (128, 128), 1)
                visible = (key_pos <= query_pos) & (key_seg == query_seg)
                bias_s[pl.ds(first, 128), pl.ds(j * 128, 128)] = jnp.where(visible, 0.0, HIDDEN)

    def long_bias():
        query_pos = lax.broadcasted_iota(jnp.int32, (LONG, LONG), 0)
        key_pos = lax.broadcasted_iota(jnp.int32, (LONG, LONG), 1)
        visible = (key_pos <= query_pos) & (key_pos + blk * LONG < len_ref[0])
        bias_l[...] = jnp.where(visible, 0.0, HIDDEN)

    def short_attention(g):
        kv = pl.ds((g // 2) * HD, HD)
        for i in range(4):
            keys = pl.ds(max(i - 2, 0) * 256, 256 * min(i + 1, 3))
            rows = pl.ds(i * 256, 256)
            for h in range(2):
                scores = lax.dot_general(
                    qb[g, rows, pl.ds(h * HD, HD)], kb[keys, kv], NT, preferred_element_type=F32
                )
                scores = scores * SCALE + bias_s[rows, pl.ds(0, 256 * min(i + 1, 3))]
                top = jnp.max(scores, axis=1, keepdims=True)
                weights = jnp.exp2(scores - top)
                total = jnp.sum(weights, axis=1, keepdims=True)
                mixed = jnp.dot(weights.astype(BF16), vb[keys, kv], preferred_element_type=F32)
                sob[g, rows, pl.ds(h * HD, HD)] = (mixed / total).astype(BF16)

    def long_step(kv, j, bias, fresh):
        keys = kvl[j // 2, j % 2, 2 * kv]
        values = kvl[j // 2, j % 2, 2 * kv + 1]
        scores = lax.dot_general(q2[...], keys, NT, preferred_element_type=F32) * SCALE + bias
        top = jnp.maximum(mx[...], jnp.max(scores, axis=1, keepdims=True))
        shrink = jnp.exp2(mx[...] - top)
        weights = jnp.exp2(scores - top)
        tot[...] = tot[...] * shrink + jnp.sum(weights, axis=1, keepdims=True)
        acc[...] = acc[...] * shrink + jnp.dot(
            weights.astype(BF16), values, preferred_element_type=F32
        )
        mx[...] = top

    def long_attention(g):
        kv = g // 2
        length = len_ref[0]
        q2[pl.ds(0, LONG), :] = qb[g, pl.ds(SEQ, LONG), pl.ds(0, HD)]
        q2[pl.ds(LONG, LONG), :] = qb[g, pl.ds(SEQ, LONG), pl.ds(HD, HD)]
        mx[...] = jnp.full_like(mx, HIDDEN)
        tot[...] = jnp.zeros_like(tot)
        acc[...] = jnp.zeros_like(acc)

        @pl.loop(0, blk)
        def _(j):
            key_pos = j * LONG + lax.broadcasted_iota(jnp.int32, (1, LONG), 1)
            long_step(kv, j, jnp.where(key_pos < length, 0.0, HIDDEN), False)

        diagonal = bias_l[...]
        long_step(kv, blk, jnp.concatenate([diagonal, diagonal], axis=0), False)
        query_pos = blk * LONG + lax.broadcasted_iota(jnp.int32, (LONG, HD), 0)
        for h in range(2):
            half = pl.ds(h * LONG, LONG)
            mixed = acc[half, :] / tot[half, :]
            lob[g, :, pl.ds(h * HD, HD)] = jnp.where(query_pos < length, mixed, 0.0).astype(BF16)

    outs = []
    peer_outs = []

    def ship_short(g):
        columns = pl.ds(pl.multiple_of(core * SEQ + g * WIDTH, WIDTH), WIDTH)
        theirs = pl.ds(pl.multiple_of((1 - core) * HALF, HALF), HALF)
        peer = pltpu.make_async_remote_copy(
            src_ref=sob.at[g, theirs], dst_ref=so_hbm.at[0, :, columns],
            send_sem=out_send.at[g], recv_sem=out_recv.at[g], device_id=sibling, device_id_type=MESH,
        )
        mine = pltpu.make_async_copy(sob.at[g, my_rows], so_hbm.at[0, :, columns], out_own.at[g])
        peer.start()
        mine.start()
        peer_outs.append(peer)
        outs.append(mine)

    def ship_long(g):
        mine = pltpu.make_async_copy(
            lob.at[g], lo_hbm.at[0, :, pl.ds(g * WIDTH, WIDTH)], out_own.at[4 + g]
        )
        mine.start()
        outs.append(mine)

    send(0, 0, False)
    peer_x.start()
    long_bias()
    arrive(0, 0, False)
    send(0, 0, True)
    short_bias()
    arrive(0, 0, True)
    send(1, 0, False)
    send(1, 1, False)
    own_x.wait()
    own_l.wait()
    arrive(1, 0, False)
    send(1, 0, True)
    arrive(1, 0, True)
    send(2, 0, False)
    arrive(1, 1, False)
    send(1, 1, True)
    send(1, 2, False)
    arrive(1, 1, True)
    send(2, 1, False)
    peer_x.wait_recv()

    def turn_one(g):
        if g + 2 < GROUPS:
            arrive(1, g + 2, False)
            send(1, g + 2, True)
        if g + 3 < GROUPS:
            send(1, g + 3, False)
        if g < GROUPS:
            arrive(2, g, False)
            send(2, g, True)

    def turn_two(g):
        if g + 2 < GROUPS:
            arrive(1, g + 2, True)
            send(2, g + 2, False)

    def turn_three(g):
        if g < GROUPS:
            arrive(2, g, True)

    turn_one(0)
    turn_two(0)
    turn_three(0)
    project(0, kb)
    turn_one(1)
    turn_two(1)
    turn_three(1)
    project(1, vb)
    for h in range(2):
        kvl[cx, yl, 2 * h] = kb[pl.ds(SEQ, LONG), pl.ds(h * HD, HD)]
        kvl[cx, yl, 2 * h + 1] = vb[pl.ds(SEQ, LONG), pl.ds(h * HD, HD)]
    turn_one(2)
    kv_start(0, 1, 2)
    turn_two(2)
    turn_three(2)
    project(2, qb.at[0])
    turn_one(3)
    kv_wait(0)
    kv_start(3, 4)
    kv_wait(1, 2)
    kv_start(5, 6)
    short_attention(0)
    ship_short(0)
    turn_two(3)
    kv_wait(5, 6)
    kv_start(9)
    kv_wait(3, 4)
    kv_start(7, 8)
    turn_three(3)
    project(3, qb.at[1])
    turn_one(4)
    short_attention(1)
    ship_short(1)
    kv_wait(7, 8)
    kv_wait(9)
    long_attention(0)
    ship_long(0)
    turn_three(4)
    project(4, qb.at[2])
    turn_one(5)
    short_attention(2)
    ship_short(2)
    long_attention(1)
    ship_long(1)
    turn_three(5)
    project(5, qb.at[3])
    short_attention(3)
    ship_short(3)
    long_attention(2)
    ship_long(2)
    long_attention(3)
    ship_long(3)

    peer_x.wait_send()
    for copy in sent:
        copy.wait_send()
    for copy in outs:
        copy.wait()
    for copy in peer_outs:
        copy.wait()


def local(short_tokens, short_segments, long_tokens, long_lengths, w_query, w_key, w_value):
    anywhere = pl.BlockSpec(memory_space=pl.ANY)
    vmem = pl.BlockSpec(memory_space=pltpu.VMEM)
    smem = pl.BlockSpec(memory_space=pltpu.SMEM)
    dma = pltpu.SemaphoreType.DMA
    return pl.pallas_call(
        kernel,
        out_shape=(
            jax.ShapeDtypeStruct((1, HALF, 2 * SEQ), BF16),
            jax.ShapeDtypeStruct((1, LONG, SEQ), BF16),
        ),
        in_specs=[anywhere, vmem, anywhere, smem, anywhere, anywhere, anywhere],
        out_specs=(anywhere, anywhere),
        scratch_shapes=[
            pltpu.VMEM((GROUPS, 4, 2, 4, 2, 64, WIDTH), BF16),
            pltpu.VMEM((ROWS, D), BF16),
            pltpu.VMEM((ROWS, WIDTH), BF16),
            pltpu.VMEM((ROWS, WIDTH), BF16),
            pltpu.VMEM((4, ROWS, WIDTH), BF16),
            pltpu.VMEM((4, 2, 4, LONG, HD), BF16),
            pltpu.VMEM((4, SEQ, WIDTH), BF16),
            pltpu.VMEM((4, LONG, WIDTH), BF16),
            pltpu.VMEM((SEQ, 768), F32),
            pltpu.VMEM((LONG, LONG), F32),
            pltpu.VMEM((2 * LONG, HD), BF16),
            pltpu.VMEM((2 * LONG, HD), F32),
            pltpu.VMEM((2 * LONG, 1), F32),
            pltpu.VMEM((2 * LONG, 1), F32),
            dma((13, 3, 4)),
            dma((13, 3, 4)),
            dma((10,)),
            dma((10,)),
            dma((4,)),
            dma((6,)),
            dma((4,)),
            dma((4,)),
            dma((8,)),
        ],
        compiler_params=pltpu.CompilerParams(
            collective_id=0, has_side_effects=True, vmem_limit_bytes=63_000_000
        ),
    )(short_tokens, short_segments, long_tokens, long_lengths, w_query, w_key, w_value)


def solution(mesh):
    return jax.shard_map(
        local,
        mesh=mesh,
        in_specs=(
            P(("blk", "dp"), "uly", None),
            P(("blk", "dp"), None),
            P("dp", "blk", None),
            P("dp"),
            P(("blk", "dp"), "uly"),
            P(("blk", "dp"), "uly"),
            P(("blk", "dp"), "uly"),
        ),
        out_specs=(P(("blk", "dp"), "uly", None), P("dp", "blk", "uly")),
        check_vma=False,
    )
```

```python
import math

import jax
import jax.numpy as jnp
from jax import lax
from jax.experimental import pallas as pl
from jax.experimental.pallas import tpu as pltpu
from jax.sharding import PartitionSpec as P

MESH = pl.DeviceIdType.MESH
BF16 = jnp.bfloat16
F32 = jnp.float32
HD = 128
D = 4096
SEQ = 1024
HALF = 512
LONG = 384
ROWS = SEQ + LONG
GROUPS = 6
WIDTH = 256
HIDDEN = -1e30
SCALE = math.log2(math.e) / math.sqrt(HD)

PARTS = ((0, 32, "xyz"), (32, 16, "yzx"), (48, 16, "zxy"))

NT = (((1,), (1,)), ((), ()))


def kernel(
    xs_hbm, seg_ref, xl_hbm, len_ref, wq_hbm, wk_hbm, wv_hbm,
    so_hbm, lo_hbm,
    w, x, kb, vb, qb, kvl, sob, lob, bias_s, bias_l, sc_s, sc_l, acc, mx, tot,
    send_sem, recv_sem, kv_send, kv_recv, x_sem, own_sem, out_send, out_recv, out_own,
):
    blk, core, dp = lax.axis_index("blk"), lax.axis_index("uly"), lax.axis_index("dp")
    cx, yl = blk // 2, blk % 2
    cz, yh = dp // 2, dp % 2
    cy = yh * 2 + yl
    here = {"x": cx, "y": cy, "z": cz}

    def device(dim, step):
        at = dict(here)
        at[dim] = (here[dim] + step + 4) % 4
        return (at["x"] * 2 + at["y"] % 2, core, at["z"] * 2 + at["y"] // 2)

    sibling = (blk, 1 - core, dp)

    own = [
        pltpu.make_async_copy(wk_hbm, w.at[0, cx, yl, cz, yh], own_sem.at[0]),
        pltpu.make_async_copy(wv_hbm, w.at[1, cx, yl, cz, yh], own_sem.at[1]),
    ]
    for g in range(4):
        own.append(
            pltpu.make_async_copy(
                wq_hbm.at[:, pl.ds(g * WIDTH, WIDTH)], w.at[2 + g, cx, yl, cz, yh], own_sem.at[2 + g]
            )
        )
    my_rows = pl.ds(pl.multiple_of(core * HALF, HALF), HALF)
    own_x = pltpu.make_async_copy(xs_hbm.at[0], x.at[my_rows], x_sem.at[0])
    own_l = pltpu.make_async_copy(xl_hbm.at[0], x.at[pl.ds(SEQ, LONG)], x_sem.at[1])
    for copy in own + [own_l, own_x]:
        copy.start()

    barrier = pltpu.get_barrier_semaphore()
    for dim in "xyz":
        for step in (1, -1):
            pl.semaphore_signal(barrier, inc=1, device_id=device(dim, step), device_id_type=MESH)
    pl.semaphore_signal(barrier, inc=1, device_id=sibling, device_id_type=MESH)
    pl.semaphore_wait(barrier, 7)

    peer_x = pltpu.make_async_remote_copy(
        src_ref=xs_hbm.at[0], dst_ref=x.at[my_rows], send_sem=x_sem.at[2], recv_sem=x_sem.at[3],
        device_id=sibling, device_id_type=MESH,
    )
    for copy in own:
        copy.wait()

    def block(groups, part, phase, position, half=None):
        first, count, order = PARTS[part]
        dim = order[phase]
        at = dict(here)
        at[dim] = position
        done = order[:phase]
        ix = slice(None) if "x" in done else at["x"]
        iz = slice(None) if "z" in done else at["z"]
        il = slice(None) if "y" in done else at["y"] % 2
        ih = slice(None) if "y" in done else at["y"] // 2
        columns = slice(None)
        if half is not None:
            if phase == 0:
                columns = pl.ds(half * 128, 128)
            elif order[0] == "x":
                ix = pl.ds(2 * half, 2)
            elif order[0] == "z":
                iz = pl.ds(2 * half, 2)
            else:
                il = half
        return w.at[groups, ix, il, iz, ih, pl.ds(first, count), columns]

    def hop(groups, stage, part, phase, slot):
        dim = PARTS[part][2][phase]
        step = 1 if slot % 2 == 0 else -1
        if slot < 2:
            ref = block(groups, part, phase, here[dim])
        else:
            ref = block(groups, part, phase, (here[dim] - step + 4) % 4, half=slot % 2)
        return pltpu.make_async_remote_copy(
            src_ref=ref, dst_ref=ref,
            send_sem=send_sem.at[stage, part, slot], recv_sem=recv_sem.at[stage, part, slot],
            device_id=device(dim, step), device_id_type=MESH,
        )

    sent = []

    def send(phase, g, second):
        groups = slice(None) if phase == 0 else g
        stage = 0 if phase == 0 else 1 + (phase - 1) * GROUPS + g
        for part in range(3):
            for slot in (2, 3) if second else (0, 1):
                copy = hop(groups, stage, part, phase, slot)
                copy.start()
                sent.append(copy)

    def arrive(phase, g, second):
        groups = slice(None) if phase == 0 else g
        stage = 0 if phase == 0 else 1 + (phase - 1) * GROUPS + g
        for part in range(3):
            for slot in (2, 3) if second else (0, 1):
                hop(groups, stage, part, phase, slot).wait_recv()

    def kv_copy(index, ref, dim, step):
        return pltpu.make_async_remote_copy(
            src_ref=ref, dst_ref=ref, send_sem=kv_send.at[index], recv_sem=kv_recv.at[index],
            device_id=device(dim, step) if dim == "x" else ((cx * 2 + 1 - yl), core, dp), device_id_type=MESH,
        )

    def kv_hops(index):
        left, right = (cx + 3) % 4, (cx + 1) % 4
        if index == 0:
            return kv_copy(0, kvl.at[cx, yl, pl.ds(0, 2)], "y", 0)
        if index in (1, 2):
            return kv_copy(index, kvl.at[cx, yl, pl.ds(2, 2)], "x", 1 if index == 1 else -1)
        if index in (3, 4):
            return kv_copy(index, kvl.at[cx, :, pl.ds(0, 2)], "x", 1 if index == 3 else -1)
        if index == 5:
            return kv_copy(5, kvl.at[left, yl, 2], "x", 1)
        if index == 6:
            return kv_copy(6, kvl.at[right, yl, 3], "x", -1)
        if index == 7:
            return kv_copy(7, kvl.at[left, 0, pl.ds(0, 2)], "x", 1)
        if index == 8:
            return kv_copy(8, kvl.at[right, 1, pl.ds(0, 2)], "x", -1)
        return kv_copy(9, kvl.at[:, yl, pl.ds(2, 2)], "y", 0)

    def kv_start(*indices):
        for index in indices:
            copy = kv_hops(index)
            copy.start()
            sent.append(copy)

    def kv_wait(*indices):
        for index in indices:
            kv_hops(index).wait_recv()

    def project(g, out):
        tile = 704

        for i in range(ROWS // tile):
            rows = pl.ds(i * tile, tile)
            out[rows, :] = jnp.dot(
                x[rows, :], w[g].reshape(D, WIDTH), preferred_element_type=F32
            ).astype(BF16)

    def short_bias():
        @pl.loop(0, 8)
        def _(i):
            first = pl.multiple_of(i * 128, 128)
            own_seg = seg_ref[:, pl.ds(first, 128)].astype(F32)
            query_seg = jnp.transpose(jnp.broadcast_to(own_seg, (128, 128)))
            window = jnp.maximum(i // 2 - 2, 0) * 256
            for j in range(6):
                start = pl.multiple_of(window + j * 128, 128)
                key_seg = jnp.broadcast_to(seg_ref[:, pl.ds(start, 128)].astype(F32), (128, 128))
                query_pos = first + lax.broadcasted_iota(jnp.int32, (128, 128), 0)
                key_pos = start + lax.broadcasted_iota(jnp.int32, (128, 128), 1)
                visible = (key_pos <= query_pos) & (key_seg == query_seg)
                bias_s[pl.ds(first, 128), pl.ds(j * 128, 128)] = jnp.where(visible, 0.0, HIDDEN)

    def long_bias():
        query_pos = yl * LONG + lax.broadcasted_iota(jnp.int32, (LONG, 2 * LONG), 0)
        key_pos = lax.broadcasted_iota(jnp.int32, (LONG, 2 * LONG), 1)
        visible = (key_pos <= query_pos) & (key_pos + cx * (2 * LONG) < len_ref[0])
        bias_l[...] = jnp.where(visible, 0.0, HIDDEN)

    def short_attention(g):
        kv = pl.ds((g // 2) * HD, HD)
        items = [(i, h) for i in range(4) for h in range(2)]

        def score(n):
            i, h = items[n]
            width = 256 * min(i + 1, 3)
            sc_s[n % 2, :, pl.ds(0, width)] = lax.dot_general(
                qb[g, pl.ds(i * 256, 256), pl.ds(h * HD, HD)],
                kb[pl.ds(max(i - 2, 0) * 256, width), kv],
                NT,
                preferred_element_type=F32,
            )

        score(0)
        for n, (i, h) in enumerate(items):
            if n + 1 < len(items):
                score(n + 1)
            width = 256 * min(i + 1, 3)
            rows = pl.ds(i * 256, 256)
            scores = sc_s[n % 2, :, pl.ds(0, width)] * SCALE + bias_s[rows, pl.ds(0, width)]
            top = jnp.max(scores, axis=1, keepdims=True)
            weights = jnp.exp2(scores - top)
            total = jnp.sum(weights, axis=1, keepdims=True)
            mixed = jnp.dot(
                weights.astype(BF16),
                vb[pl.ds(max(i - 2, 0) * 256, width), kv],
                preferred_element_type=F32,
            )
            sob[g, rows, pl.ds(h * HD, HD)] = (mixed / total).astype(BF16)

    def tiles(value):
        return [value[:, t * HD : (t + 1) * HD] for t in range(value.shape[1] // HD)]

    def fold(op, value):
        parts = tiles(value)
        while len(parts) > 1:
            parts = [
                op(parts[n], parts[n + 1]) if n + 1 < len(parts) else parts[n]
                for n in range(0, len(parts), 2)
            ]
        return parts[0]

    def pair(j, which):
        return jnp.concatenate([kvl[j, 0, which], kvl[j, 1, which]], axis=0)

    def long_score(g, h, j, bias):
        scores = bias + lax.dot_general(
            qb[g, pl.ds(SEQ, LONG), pl.ds(h * HD, HD)],
            pair(j, 2 * (g // 2)),
            NT,
            preferred_element_type=F32,
        )
        sc_l[h, j] = scores
        mx[h] = jnp.maximum(mx[h], fold(jnp.maximum, scores))

    def long_mix(g, h, j):
        top = mx[h]
        weights = jnp.exp2(sc_l[h, j] * SCALE - jnp.concatenate([top] * 6, axis=1))
        tot[h] += fold(jnp.add, weights)
        acc[h] += jnp.dot(
            weights.astype(BF16), pair(j, 2 * (g // 2) + 1), preferred_element_type=F32
        )

    def long_attention(g):
        length = len_ref[0]
        mx[...] = jnp.full_like(mx, HIDDEN)
        tot[...] = jnp.zeros_like(tot)
        acc[...] = jnp.zeros_like(acc)

        def row_bias(j):
            key_pos = j * (2 * LONG) + lax.broadcasted_iota(jnp.int32, (1, 2 * LONG), 1)
            return jnp.where(key_pos < length, 0.0, HIDDEN)

        def top(h):
            mx[h] = jnp.broadcast_to(jnp.max(mx[h], axis=1, keepdims=True) * SCALE, (LONG, HD))

        def finish(h):
            query_pos = blk * LONG + lax.broadcasted_iota(jnp.int32, (LONG, HD), 0)
            mixed = acc[h] / jnp.sum(tot[h], axis=1, keepdims=True)
            lob[g, :, pl.ds(h * HD, HD)] = jnp.where(query_pos < length, mixed, 0.0).astype(BF16)

        @pl.loop(0, cx)
        def _(j):
            long_score(g, 0, j, row_bias(j))

        long_score(g, 0, cx, bias_l[...])
        top(0)

        @pl.loop(0, cx)
        def _(j):
            long_score(g, 1, j, row_bias(j))
            long_mix(g, 0, j)

        long_score(g, 1, cx, bias_l[...])
        long_mix(g, 0, cx)
        top(1)
        finish(0)

        @pl.loop(0, cx + 1)
        def _(j):
            long_mix(g, 1, j)

        finish(1)

    outs = []
    peer_outs = []

    def ship_short(g):
        columns = pl.ds(pl.multiple_of(core * SEQ + g * WIDTH, WIDTH), WIDTH)
        theirs = pl.ds(pl.multiple_of((1 - core) * HALF, HALF), HALF)
        peer = pltpu.make_async_remote_copy(
            src_ref=sob.at[g, theirs], dst_ref=so_hbm.at[0, :, columns],
            send_sem=out_send.at[g], recv_sem=out_recv.at[g], device_id=sibling, device_id_type=MESH,
        )
        mine = pltpu.make_async_copy(sob.at[g, my_rows], so_hbm.at[0, :, columns], out_own.at[g])
        peer.start()
        mine.start()
        peer_outs.append(peer)
        outs.append(mine)

    def ship_long(g):
        mine = pltpu.make_async_copy(
            lob.at[g], lo_hbm.at[0, :, pl.ds(g * WIDTH, WIDTH)], out_own.at[4 + g]
        )
        mine.start()
        outs.append(mine)

    send(0, 0, False)
    peer_x.start()
    long_bias()
    arrive(0, 0, False)
    send(0, 0, True)
    short_bias()
    arrive(0, 0, True)
    send(1, 0, False)
    send(1, 1, False)
    own_x.wait()
    own_l.wait()
    arrive(1, 0, False)
    send(1, 0, True)
    arrive(1, 0, True)
    send(2, 0, False)
    arrive(1, 1, False)
    send(1, 1, True)
    send(1, 2, False)
    arrive(1, 1, True)
    send(2, 1, False)
    peer_x.wait_recv()

    def turn_one(g):
        if g + 2 < GROUPS:
            arrive(1, g + 2, False)
            send(1, g + 2, True)
        if g + 3 < GROUPS:
            send(1, g + 3, False)
        if g < GROUPS:
            arrive(2, g, False)
            send(2, g, True)

    def turn_two(g):
        if g + 2 < GROUPS:
            arrive(1, g + 2, True)
            send(2, g + 2, False)

    def turn_three(g):
        if g < GROUPS:
            arrive(2, g, True)

    turn_one(0)
    turn_two(0)
    turn_three(0)
    project(0, kb)
    turn_one(1)
    turn_two(1)
    turn_three(1)
    project(1, vb)
    for h in range(2):
        kvl[cx, yl, 2 * h] = kb[pl.ds(SEQ, LONG), pl.ds(h * HD, HD)]
        kvl[cx, yl, 2 * h + 1] = vb[pl.ds(SEQ, LONG), pl.ds(h * HD, HD)]
    turn_one(2)
    kv_start(0, 1, 2)
    turn_two(2)
    turn_three(2)
    project(2, qb.at[0])
    turn_one(3)
    kv_wait(0)
    kv_start(3, 4)
    kv_wait(1, 2)
    kv_start(5, 6)
    short_attention(0)
    ship_short(0)
    turn_two(3)
    kv_wait(5, 6)
    kv_start(9)
    kv_wait(3, 4)
    kv_start(7, 8)
    turn_three(3)
    project(3, qb.at[1])
    turn_one(4)
    short_attention(1)
    ship_short(1)
    kv_wait(7, 8)
    kv_wait(9)
    long_attention(0)
    ship_long(0)
    turn_three(4)
    project(4, qb.at[2])
    turn_one(5)
    short_attention(2)
    ship_short(2)
    long_attention(1)
    ship_long(1)
    turn_three(5)
    project(5, qb.at[3])
    short_attention(3)
    ship_short(3)
    long_attention(2)
    ship_long(2)
    long_attention(3)
    ship_long(3)

    peer_x.wait_send()
    for copy in sent:
        copy.wait_send()
    for copy in outs:
        copy.wait()
    for copy in peer_outs:
        copy.wait()


def local(short_tokens, short_segments, long_tokens, long_lengths, w_query, w_key, w_value):
    anywhere = pl.BlockSpec(memory_space=pl.ANY)
    vmem = pl.BlockSpec(memory_space=pltpu.VMEM)
    smem = pl.BlockSpec(memory_space=pltpu.SMEM)
    dma = pltpu.SemaphoreType.DMA
    return pl.pallas_call(
        kernel,
        out_shape=(
            jax.ShapeDtypeStruct((1, HALF, 2 * SEQ), BF16),
            jax.ShapeDtypeStruct((1, LONG, SEQ), BF16),
        ),
        in_specs=[anywhere, vmem, anywhere, smem, anywhere, anywhere, anywhere],
        out_specs=(anywhere, anywhere),
        scratch_shapes=[
            pltpu.VMEM((GROUPS, 4, 2, 4, 2, 64, WIDTH), BF16),
            pltpu.VMEM((ROWS, D), BF16),
            pltpu.VMEM((ROWS, WIDTH), BF16),
            pltpu.VMEM((ROWS, WIDTH), BF16),
            pltpu.VMEM((4, ROWS, WIDTH), BF16),
            pltpu.VMEM((4, 2, 4, LONG, HD), BF16),
            pltpu.VMEM((4, SEQ, WIDTH), BF16),
            pltpu.VMEM((4, LONG, WIDTH), BF16),
            pltpu.VMEM((SEQ, 768), F32),
            pltpu.VMEM((LONG, 2 * LONG), F32),
            pltpu.VMEM((2, 256, 768), F32),
            pltpu.VMEM((2, 4, LONG, 2 * LONG), F32),
            pltpu.VMEM((2, LONG, HD), F32),
            pltpu.VMEM((2, LONG, HD), F32),
            pltpu.VMEM((2, LONG, HD), F32),
            dma((13, 3, 4)),
            dma((13, 3, 4)),
            dma((10,)),
            dma((10,)),
            dma((4,)),
            dma((6,)),
            dma((4,)),
            dma((4,)),
            dma((8,)),
        ],
        compiler_params=pltpu.CompilerParams(
            collective_id=0, has_side_effects=True, vmem_limit_bytes=60_000_000
        ),
    )(short_tokens, short_segments, long_tokens, long_lengths, w_query, w_key, w_value)


def solution(mesh):
    return jax.shard_map(
        local,
        mesh=mesh,
        in_specs=(
            P(("blk", "dp"), "uly", None),
            P(("blk", "dp"), None),
            P("dp", "blk", None),
            P("dp"),
            P(("blk", "dp"), "uly"),
            P(("blk", "dp"), "uly"),
            P(("blk", "dp"), "uly"),
        ),
        out_specs=(P(("blk", "dp"), "uly", None), P("dp", "blk", "uly")),
        check_vma=False,
    )
```

```python
import math

import jax
import jax.numpy as jnp
from jax import lax
from jax.experimental import pallas as pl
from jax.experimental.pallas import tpu as pltpu
from jax.sharding import PartitionSpec as P

MESH = pl.DeviceIdType.MESH
BF16 = jnp.bfloat16
F32 = jnp.float32
HD = 128
D = 4096
SEQ = 1024
HALF = 512
LONG = 384
ROWS = SEQ + LONG
TILE = ROWS // 2
GROUPS = 6
WIDTH = 256
HIDDEN = -1e30
VMEM = 60_000_000
SCALE = math.log2(math.e) / math.sqrt(HD)

ORDERS = ("xyz", "yzx", "zxy")
PARTS = (
    ((0, 32), (32, 16), (48, 16)),
    ((0, 16), (16, 16), (32, 32)),
    ((0, 32), (32, 16), (48, 16)),
    ((0, 32), (32, 16), (48, 16)),
    ((0, 16), (16, 32), (48, 16)),
    ((0, 16), (16, 32), (48, 16)),
)
FIRST = ((0,), (1,), (2, 3), (4, 5),)
ORDER = (
    "P0a01", "P0a02", "P0a00", "P0a20", "P0a21", "P0a12", "P0a11", "P0a42", "P0a10", "P0a40", "B", "P0a41", "P0a22",
    "P0b02", "P0b01", "P0b00", "P0b12", "P0b21", "P0b11", "P0b42", "P0b20", "P0b10", "P0b22", "P0b41", "P0b40",
    "P1a02", "P1a01", "P1a00", "P1a12", "P1a21", "P1a31", "P1a11", "P1a52", "P1a42", "P1a22", "P1a30", "P1a32",
    "P1a10", "P1a41", "P1a40", "P1b02", "P1b01", "P1b21", "P1b00", "P1b12", "P1b31", "P1a51", "P1b11", "P1b52",
    "P1a50", "P1b30", "P1b42", "P1b10", "P1b41", "P1b22", "P1b40", "P2a01", "P2a21", "P1b32", "P1a20", "P2a00",
    "P2a31", "P2a02", "P1b50", "P2a12", "P2a10", "P2a11", "P2a41", "P2a42", "P2a40", "P2b01", "P1b20", "P2b02",
    "P2b21", "P2a32", "P2b00", "P2b31", "P2b10", "P2b12", "P2a30", "P2b11", "P2b40", "P2b42", "P2a22", "P2a20",
    "P2b41", "P2b32", "W0", "X", "pr01", "K2", "K1", "pr00", "P2b30", "W1", "pr11", "V1", "V2", "pr10", "P2b22",
    "W4", "pr4", "P2b20", "sh2", "P1b51", "K3", "W3", "pr3", "V4", "V3", "P2a50", "sh1", "W2", "P2a51", "lo1own",
    "K5", "lo2own", "pr2", "P2b50", "V5", "sh0", "K4", "lo0own", "P2b51", "lo0near", "P2a52", "lo0far", "lo2near",
    "lo2far", "lo1near", "lo0other", "P2b52", "lo2other", "lo1far", "lo1other", "W5", "pr5", "sh3", "lo3own",
    "lo3near", "lo3far", "lo3other",
)

NT = (((1,), (1,)), ((), ()))


def kernel(
    xs_hbm, seg_ref, xl_hbm, len_ref, wq_hbm, wk_hbm, wv_hbm,
    so_hbm, lo_hbm,
    w, x, kb, vb, qb, kvl, sob, lob, bias_s, bias_l, sc_s, sc_l, acc, mx, tot,
    send_sem, recv_sem, kv_send, kv_recv, x_sem, own_sem, out_send, out_recv, out_own,
):
    blk, core, dp = lax.axis_index("blk"), lax.axis_index("uly"), lax.axis_index("dp")
    cx, yl = blk // 2, blk % 2
    cz, yh = dp // 2, dp % 2
    cy = yh * 2 + yl
    here = {"x": cx, "y": cy, "z": cz}

    def device(dim, step):
        at = dict(here)
        at[dim] = (here[dim] + step + 4) % 4
        return (at["x"] * 2 + at["y"] % 2, core, at["z"] * 2 + at["y"] // 2)

    sibling = (blk, 1 - core, dp)

    own = [
        pltpu.make_async_copy(wk_hbm, w.at[0, cx, yl, cz, yh], own_sem.at[0]),
        pltpu.make_async_copy(wv_hbm, w.at[1, cx, yl, cz, yh], own_sem.at[1]),
    ]
    for g in range(4):
        own.append(
            pltpu.make_async_copy(
                wq_hbm.at[:, pl.ds(g * WIDTH, WIDTH)], w.at[2 + g, cx, yl, cz, yh], own_sem.at[2 + g]
            )
        )
    my_rows = pl.ds(pl.multiple_of(core * HALF, HALF), HALF)
    own_x = pltpu.make_async_copy(xs_hbm.at[0], x.at[my_rows], x_sem.at[0])
    own_l = pltpu.make_async_copy(xl_hbm.at[0], x.at[pl.ds(SEQ, LONG)], x_sem.at[1])
    for copy in own + [own_l, own_x]:
        copy.start()

    barrier = pltpu.get_barrier_semaphore()
    for dim in "xyz":
        for step in (1, -1):
            pl.semaphore_signal(barrier, inc=1, device_id=device(dim, step), device_id_type=MESH)
    pl.semaphore_signal(barrier, inc=1, device_id=sibling, device_id_type=MESH)
    pl.semaphore_wait(barrier, 7)

    peer_x = pltpu.make_async_remote_copy(
        src_ref=xs_hbm.at[0], dst_ref=x.at[my_rows], send_sem=x_sem.at[2], recv_sem=x_sem.at[3],
        device_id=sibling, device_id_type=MESH,
    )
    for copy in own:
        copy.wait()

    def block(groups, part, phase, position, half=None):
        first, count = PARTS[groups[0]][part]
        order = ORDERS[part]
        at = dict(here)
        at[order[phase]] = position
        done = order[:phase]
        ix = slice(None) if "x" in done else at["x"]
        iz = slice(None) if "z" in done else at["z"]
        il = slice(None) if "y" in done else at["y"] % 2
        ih = slice(None) if "y" in done else at["y"] // 2
        columns = slice(None)
        if half is not None:
            if phase == 0:
                columns = pl.ds(half * 128, 128)
            elif order[0] == "x":
                ix = pl.ds(2 * half, 2)
            elif order[0] == "z":
                iz = pl.ds(2 * half, 2)
            else:
                il = half
        which = pl.ds(groups[0], len(groups)) if len(groups) > 1 else groups[0]
        return w.at[which, ix, il, iz, ih, pl.ds(first, count), columns]

    def hop(groups, part, phase, slot):
        dim = ORDERS[part][phase]
        step = 1 if slot % 2 == 0 else -1
        if slot < 2:
            ref = block(groups, part, phase, here[dim])
        else:
            ref = block(groups, part, phase, (here[dim] - step + 4) % 4, half=slot % 2)
        stage = phase * GROUPS + groups[0]
        return pltpu.make_async_remote_copy(
            src_ref=ref, dst_ref=ref,
            send_sem=send_sem.at[stage, part, slot], recv_sem=recv_sem.at[stage, part, slot],
            device_id=device(dim, step), device_id_type=MESH,
        )

    sent = []

    def start(copy):
        copy.start()
        sent.append(copy)

    def send(groups, part, phase, second):
        for slot in (2, 3) if second else (0, 1):
            start(hop(groups, part, phase, slot))

    def arrive(groups, part, phase, second):
        for slot in (2, 3) if second else (0, 1):
            hop(groups, part, phase, slot).wait_recv()

    near, far = (cx + 3) % 4, (cx + 1) % 4
    other = (cx + 2) % 4
    keys, vals = pl.ds(0, 2), pl.ds(2, 2)
    kv_table = (
        ("y", kvl.at[cx, yl, keys]),
        ("x+", kvl.at[cx, yl, keys]),
        ("x-", kvl.at[cx, yl, keys]),
        ("x+", kvl.at[cx, 1 - yl, keys]),
        ("x-", kvl.at[cx, 1 - yl, keys]),
        ("x+", kvl.at[near, yl, keys]),
        ("x-", kvl.at[far, 1 - yl, keys]),
        ("x+", kvl.at[cx, yl, vals]),
        ("x-", kvl.at[cx, yl, vals]),
        ("y", kvl.at[cx, yl, vals]),
        ("x+", kvl.at[near, yl, 2]),
        ("x-", kvl.at[far, yl, 3]),
        ("y", kvl.at[near, yl, vals]),
        ("y", kvl.at[far, yl, vals]),
        ("y", kvl.at[other, yl, vals]),
    )

    def kv_hop(index):
        way, ref = kv_table[index]
        to = (cx * 2 + 1 - yl, core, dp) if way == "y" else device("x", 1 if way == "x+" else -1)
        return pltpu.make_async_remote_copy(
            src_ref=ref, dst_ref=ref, send_sem=kv_send.at[index], recv_sem=kv_recv.at[index],
            device_id=to, device_id_type=MESH,
        )

    kv_steps = {
        "K1": ((0,), ()),
        "K2": ((1, 2), ()),
        "K3": ((3, 4), (0,)),
        "K4": ((5,), (1,)),
        "K5": ((6,), (4,)),
        "V1": ((7, 8), ()),
        "V2": ((9,), ()),
        "V3": ((10, 11), (7, 8)),
        "V4": ((12, 13), (7, 8)),
        "V5": ((14,), (10, 11)),
    }
    kv_needs = {"own": (0, 9), "near": (1, 3, 7, 12), "far": (2, 4, 8, 13), "other": (5, 6, 10, 11, 14)}
    arrived = set()

    def kv_wait(indices):
        for index in indices:
            if index not in arrived:
                arrived.add(index)
                kv_hop(index).wait_recv()

    def rows_of(g, rows):
        return jnp.dot(x[rows, :], w[g].reshape(D, WIDTH), preferred_element_type=F32).astype(BF16)

    def project_kv(g, tile):
        @pl.when(core < 2)
        def _():
            rows = pl.ds(tile * TILE, TILE)
            result = rows_of(g, rows)
            (kb, vb)[g][rows, :] = result
            if tile == 1:
                for h in range(2):
                    kvl[cx, yl, 2 * g + h] = result[SEQ - TILE :, h * HD : (h + 1) * HD]

    def project_q(g):
        @pl.loop(0, ROWS // TILE)
        def _(i):
            rows = pl.ds(pl.multiple_of(i * TILE, 64), TILE)
            qb[g, rows, :] = rows_of(g + 2, rows)

    def short_bias():
        @pl.loop(0, 8)
        def _(i):
            first = pl.multiple_of(i * 128, 128)
            own_seg = seg_ref[:, pl.ds(first, 128)].astype(F32)
            query_seg = jnp.transpose(jnp.broadcast_to(own_seg, (128, 128)))
            window = jnp.maximum(i // 2 - 2, 0) * 256
            for j in range(6):
                start = pl.multiple_of(window + j * 128, 128)
                key_seg = jnp.broadcast_to(seg_ref[:, pl.ds(start, 128)].astype(F32), (128, 128))
                query_pos = first + lax.broadcasted_iota(jnp.int32, (128, 128), 0)
                key_pos = start + lax.broadcasted_iota(jnp.int32, (128, 128), 1)
                visible = (key_pos <= query_pos) & (key_seg == query_seg)
                bias_s[pl.ds(first, 128), pl.ds(j * 128, 128)] = jnp.where(visible, 0.0, HIDDEN)

    def long_bias():
        query_pos = yl * LONG + lax.broadcasted_iota(jnp.int32, (LONG, 2 * LONG), 0)
        key_pos = lax.broadcasted_iota(jnp.int32, (LONG, 2 * LONG), 1)
        visible = (key_pos <= query_pos) & (key_pos + cx * (2 * LONG) < len_ref[0])
        bias_l[...] = jnp.where(visible, 0.0, HIDDEN)

    def short_attention(g):
        kv = pl.ds((g // 2) * HD, HD)

        @pl.loop(0, 2)
        def _(h):
            head = pl.ds(pl.multiple_of(h * HD, HD), HD)

            def score(i):
                width = 256 * min(i + 1, 3)
                sc_s[i % 2, :, pl.ds(0, width)] = lax.dot_general(
                    qb[g, pl.ds(i * 256, 256), head],
                    kb[pl.ds(max(i - 2, 0) * 256, width), kv],
                    NT,
                    preferred_element_type=F32,
                )

            score(0)
            for i in range(4):
                if i < 3:
                    score(i + 1)
                width = 256 * min(i + 1, 3)
                rows = pl.ds(i * 256, 256)
                scores = sc_s[i % 2, :, pl.ds(0, width)] * SCALE + bias_s[rows, pl.ds(0, width)]
                top = jnp.max(scores, axis=1, keepdims=True)
                weights = jnp.exp2(scores - top)
                total = jnp.sum(weights, axis=1, keepdims=True)
                mixed = jnp.dot(
                    weights.astype(BF16),
                    vb[pl.ds(max(i - 2, 0) * 256, width), kv],
                    preferred_element_type=F32,
                )
                sob[g, rows, head] = (mixed / total).astype(BF16)

    def tiles(value):
        return [value[:, t * HD : (t + 1) * HD] for t in range(value.shape[1] // HD)]

    def fold(op, value):
        parts = tiles(value)
        while len(parts) > 1:
            parts = [
                op(parts[n], parts[n + 1]) if n + 1 < len(parts) else parts[n]
                for n in range(0, len(parts), 2)
            ]
        return parts[0]

    def pair(j, which):
        return jnp.concatenate([kvl[j, 0, which], kvl[j, 1, which]], axis=0)

    def long_part(g, j, bias, fresh):
        kv = g // 2
        for h in range(2):
            sc_l[h] = bias + lax.dot_general(
                qb[g, pl.ds(SEQ, LONG), pl.ds(h * HD, HD)], pair(j, kv), NT, preferred_element_type=F32
            )
        for h in range(2):
            n = 2 * g + h
            largest = jnp.max(fold(jnp.maximum, sc_l[h]), axis=1, keepdims=True) * SCALE
            top = jnp.broadcast_to(largest, (LONG, HD))
            if not fresh:
                top = jnp.maximum(mx[n], top)
            weights = jnp.exp2(sc_l[h] * SCALE - jnp.concatenate([top] * 6, axis=1))
            mixed = jnp.dot(weights.astype(BF16), pair(j, 2 + kv), preferred_element_type=F32)
            if fresh:
                tot[n] = fold(jnp.add, weights)
                acc[n] = mixed
            else:
                shrink = jnp.exp2(mx[n] - top)
                tot[n] = tot[n] * shrink + fold(jnp.add, weights)
                acc[n] = acc[n] * shrink + mixed
            mx[n] = top

    def long_own(g):
        long_part(g, cx, bias_l[...], True)

    def long_before(g, j):
        @pl.when(j < cx)
        def _():
            key_pos = j * (2 * LONG) + lax.broadcasted_iota(jnp.int32, (1, 2 * LONG), 1)
            long_part(g, j, jnp.where(key_pos < len_ref[0], 0.0, HIDDEN), False)

    def long_finish(g):
        query_pos = blk * LONG + lax.broadcasted_iota(jnp.int32, (LONG, HD), 0)
        for h in range(2):
            mixed = acc[2 * g + h] / jnp.sum(tot[2 * g + h], axis=1, keepdims=True)
            mixed = jnp.where(query_pos < len_ref[0], mixed, 0.0)
            lob[g, :, pl.ds(h * HD, HD)] = mixed.astype(BF16)

    outs = []
    peer_outs = []

    def ship_short(g):
        columns = pl.ds(pl.multiple_of(core * SEQ + g * WIDTH, WIDTH), WIDTH)
        theirs = pl.ds(pl.multiple_of((1 - core) * HALF, HALF), HALF)
        peer = pltpu.make_async_remote_copy(
            src_ref=sob.at[g, theirs], dst_ref=so_hbm.at[0, :, columns],
            send_sem=out_send.at[g], recv_sem=out_recv.at[g], device_id=sibling, device_id_type=MESH,
        )
        mine = pltpu.make_async_copy(sob.at[g, my_rows], so_hbm.at[0, :, columns], out_own.at[g])
        peer.start()
        mine.start()
        peer_outs.append(peer)
        outs.append(mine)

    def ship_long(g):
        mine = pltpu.make_async_copy(
            lob.at[g], lo_hbm.at[0, :, pl.ds(g * WIDTH, WIDTH)], out_own.at[4 + g]
        )
        mine.start()
        outs.append(mine)

    groups_of = {g: groups for groups in FIRST for g in groups}
    parts_of = [[p for p in range(3) if PARTS[g][p][1]] for g in range(GROUPS)]

    def step(name):
        kind, rest = name[:2], name[2:]
        if kind[0] == "P":
            phase, second, g, part = int(kind[1]), rest[0] == "b", int(rest[1]), int(rest[2])
            groups = groups_of[g] if phase == 0 else (g,)
            if second:
                arrive(groups, part, phase, False)
            elif phase == 1:
                arrive_first(g, part)
            elif phase == 2:
                arrive(groups, part, 1, True)
            send(groups, part, phase, second)
        elif kind[0] in "KV":
            sends, needs = kv_steps[name]
            kv_wait(needs)
            for index in sends:
                start(kv_hop(index))
        elif kind[0] == "W":
            g = int(kind[1])
            for part in parts_of[g]:
                arrive((g,), part, 2, True)
        elif kind == "pr":
            if len(rest) == 2:
                project_kv(int(rest[0]), int(rest[1]))
            else:
                project_q(int(rest) - 2)
        elif kind == "sh":
            short_attention(int(rest))
            ship_short(int(rest))
        elif kind == "lo":
            g, which = int(rest[0]), rest[1:]
            kv_wait(kv_needs[which])
            if which == "own":
                long_own(g)
            else:
                long_before(g, {"near": near, "far": far, "other": other}[which])
            if which == "other":
                long_finish(g)
                ship_long(g)
        elif name == "X":
            own_x.wait()
            own_l.wait()
            peer_x.wait_recv()
        else:
            peer_x.start()
            long_bias()
            short_bias()

    met = set()

    def arrive_first(g, part):
        groups = groups_of[g]
        if (groups, part) not in met:
            met.add((groups, part))
            arrive(groups, part, 0, True)

    for name in ORDER:
        step(name)

    peer_x.wait_send()
    for copy in sent:
        copy.wait_send()
    for copy in outs:
        copy.wait()
    for copy in peer_outs:
        copy.wait()


def local(short_tokens, short_segments, long_tokens, long_lengths, w_query, w_key, w_value):
    anywhere = pl.BlockSpec(memory_space=pl.ANY)
    vmem = pl.BlockSpec(memory_space=pltpu.VMEM)
    smem = pl.BlockSpec(memory_space=pltpu.SMEM)
    dma = pltpu.SemaphoreType.DMA
    return pl.pallas_call(
        kernel,
        out_shape=(
            jax.ShapeDtypeStruct((1, HALF, 2 * SEQ), BF16),
            jax.ShapeDtypeStruct((1, LONG, SEQ), BF16),
        ),
        in_specs=[anywhere, vmem, anywhere, smem, anywhere, anywhere, anywhere],
        out_specs=(anywhere, anywhere),
        scratch_shapes=[
            pltpu.VMEM((GROUPS, 4, 2, 4, 2, 64, WIDTH), BF16),
            pltpu.VMEM((ROWS, D), BF16),
            pltpu.VMEM((ROWS, WIDTH), BF16),
            pltpu.VMEM((ROWS, WIDTH), BF16),
            pltpu.VMEM((4, ROWS, WIDTH), BF16),
            pltpu.VMEM((4, 2, 4, LONG, HD), BF16),
            pltpu.VMEM((4, SEQ, WIDTH), BF16),
            pltpu.VMEM((4, LONG, WIDTH), BF16),
            pltpu.VMEM((SEQ, 768), F32),
            pltpu.VMEM((LONG, 2 * LONG), F32),
            pltpu.VMEM((2, 256, 768), F32),
            pltpu.VMEM((2, LONG, 2 * LONG), F32),
            pltpu.VMEM((8, LONG, HD), F32),
            pltpu.VMEM((8, LONG, HD), F32),
            pltpu.VMEM((8, LONG, HD), F32),
            dma((18, 3, 4)),
            dma((18, 3, 4)),
            dma((15,)),
            dma((15,)),
            dma((4,)),
            dma((6,)),
            dma((4,)),
            dma((4,)),
            dma((8,)),
        ],
        compiler_params=pltpu.CompilerParams(
            collective_id=0, has_side_effects=True, vmem_limit_bytes=VMEM
        ),
    )(short_tokens, short_segments, long_tokens, long_lengths, w_query, w_key, w_value)


def solution(mesh):
    return jax.shard_map(
        local,
        mesh=mesh,
        in_specs=(
            P(("blk", "dp"), "uly", None),
            P(("blk", "dp"), None),
            P("dp", "blk", None),
            P("dp"),
            P(("blk", "dp"), "uly"),
            P(("blk", "dp"), "uly"),
            P(("blk", "dp"), "uly"),
        ),
        out_specs=(P(("blk", "dp"), "uly", None), P("dp", "blk", "uly")),
        check_vma=False,
    )
```

```python
import math

import jax
import jax.numpy as jnp
from jax import lax
from jax.experimental import pallas as pl
from jax.experimental.pallas import tpu as pltpu
from jax.sharding import PartitionSpec as P

MESH = pl.DeviceIdType.MESH
BF16 = jnp.bfloat16
F32 = jnp.float32
HD = 128
D = 4096
SEQ = 1024
HALF = 512
LONG = 384
ROWS = SEQ + LONG
TILE = ROWS // 2
GROUPS = 6
WIDTH = 256
HIDDEN = -1e30
POOL = 40
VMEM = 60_000_000
SCALE = math.log2(math.e) / math.sqrt(HD)

ORDERS = ("xyz", "yzx", "zxy")
PARTS = (
    ((0, 32), (32, 16), (48, 16)),
    ((0, 16), (16, 16), (32, 32)),
    ((0, 32), (32, 16), (48, 16)),
    ((0, 32), (32, 16), (48, 16)),
    ((0, 16), (16, 32), (48, 16)),
    ((0, 16), (16, 32), (48, 16)),
)
FIRST = ((0,), (1,), (2, 3), (4, 5),)
ORDER = (
    "P0a01", "P0a02", "P0a00", "P0a20", "P0a21", "P0a12", "P0a11", "P0a42", "P0a10", "P0a40", "B", "P0a41", "P0a22",
    "P0b02", "P0b01", "P0b00", "P0b12", "P0b21", "P0b11", "P0b42", "P0b20", "P0b10", "P0b22", "P0b41", "P0b40",
    "P1a02", "P1a01", "P1a00", "P1a12", "P1a21", "P1a31", "P1a11", "P1a52", "P1a42", "P1a22", "P1a30", "P1a32",
    "P1a10", "P1a41", "P1a40", "P1b02", "P1b01", "P1b21", "P1b00", "P1b12", "P1b31", "P1a51", "P1b11", "P1b52",
    "P1a50", "P1b30", "P1b42", "P1b10", "P1b41", "P1b22", "P1b40", "P2a01", "P2a21", "P1b32", "P1a20", "P2a00",
    "P2a31", "P2a02", "P1b50", "P2a12", "P2a10", "P2a11", "P2a41", "P2a42", "P2a40", "P2b01", "P1b20", "P2b02",
    "P2b21", "P2a32", "P2b00", "P2b31", "P2b10", "P2b12", "P2a30", "P2b11", "P2b40", "P2b42", "P2a22", "P2a20",
    "P2b41", "P2b32", "W0", "X", "pr01", "K2", "K1", "pr00", "P2b30", "W1", "pr11", "V1", "V2", "pr10", "P2b22",
    "W4", "pr4", "P2b20", "sh2", "P1b51", "K3", "W3", "pr3", "V4", "V3", "P2a50", "sh1", "W2", "P2a51", "lo1o",
    "K5", "lo2o", "pr2", "P2b50", "V5", "sh0", "K4", "lo0o", "P2b51", "P2a52", "lo0nf", "lo2nf", "lo0t", "P2b52",
    "lo2t", "lo1nft", "W5", "pr5", "sh3", "lo3onft",
)

NT = (((1,), (1,)), ((), ()))


def kernel(
    xs_hbm, seg_ref, xl_hbm, len_ref, wq_hbm, wk_hbm, wv_hbm,
    so_hbm, lo_hbm,
    w, x, kb, vb, qb, kvl, sob, lob, bias_s, bias_l, sc_s, sc_l, acc, mx, tot,
    send_sem, recv_sem, kv_send, kv_recv, x_sem, own_sem, out_send, out_recv, out_own,
):
    blk, core, dp = lax.axis_index("blk"), lax.axis_index("uly"), lax.axis_index("dp")
    cx, yl = blk // 2, blk % 2
    cz, yh = dp // 2, dp % 2
    cy = yh * 2 + yl
    here = {"x": cx, "y": cy, "z": cz}

    def device(dim, step):
        at = dict(here)
        at[dim] = (here[dim] + step + 4) % 4
        return (at["x"] * 2 + at["y"] % 2, core, at["z"] * 2 + at["y"] // 2)

    sibling = (blk, 1 - core, dp)

    own = [
        pltpu.make_async_copy(wk_hbm, w.at[0, cx, yl, cz, yh], own_sem.at[0]),
        pltpu.make_async_copy(wv_hbm, w.at[1, cx, yl, cz, yh], own_sem.at[1]),
    ]
    for g in range(4):
        own.append(
            pltpu.make_async_copy(
                wq_hbm.at[:, pl.ds(g * WIDTH, WIDTH)], w.at[2 + g, cx, yl, cz, yh], own_sem.at[2 + g]
            )
        )
    my_rows = pl.ds(pl.multiple_of(core * HALF, HALF), HALF)
    own_x = pltpu.make_async_copy(xs_hbm.at[0], x.at[my_rows], x_sem.at[0])
    own_l = pltpu.make_async_copy(xl_hbm.at[0], x.at[pl.ds(SEQ, LONG)], x_sem.at[1])
    for copy in own + [own_l, own_x]:
        copy.start()

    barrier = pltpu.get_barrier_semaphore()
    for dim in "xyz":
        for step in (1, -1):
            pl.semaphore_signal(barrier, inc=1, device_id=device(dim, step), device_id_type=MESH)
    pl.semaphore_signal(barrier, inc=1, device_id=sibling, device_id_type=MESH)
    pl.semaphore_wait(barrier, 7)

    peer_x = pltpu.make_async_remote_copy(
        src_ref=xs_hbm.at[0], dst_ref=x.at[my_rows], send_sem=x_sem.at[2], recv_sem=x_sem.at[3],
        device_id=sibling, device_id_type=MESH,
    )
    for copy in own:
        copy.wait()

    def block(groups, part, phase, position, half=None, both=False):
        first, count = PARTS[groups[0]][part]
        order = ORDERS[part]
        dim = order[phase]
        at = dict(here)
        at[dim] = position
        done = order[:phase]
        ix = slice(None) if "x" in done else at["x"]
        iz = slice(None) if "z" in done else at["z"]
        il = slice(None) if "y" in done else at["y"] % 2
        ih = slice(None) if "y" in done else at["y"] // 2
        columns = slice(None)
        if both:
            two = pl.ds(0, 2)
            ix, il, iz = two if dim == "x" else ix, two if dim == "y" else il, two if dim == "z" else iz
        if half is not None:
            if phase == 0:
                columns = pl.ds(half * 128, 128)
            elif order[0] == "x":
                ix = pl.ds(2 * half, 2)
            elif order[0] == "z":
                iz = pl.ds(2 * half, 2)
            else:
                il = half
        which = pl.ds(groups[0], len(groups)) if len(groups) > 1 else groups[0]
        return w.at[which, ix, il, iz, ih, pl.ds(first, count), columns]

    stage_of = {}
    sent = []
    held = [None] * POOL

    def stage(groups, part, phase, second):
        return stage_of.setdefault((groups, part, phase, second), len(stage_of))

    def remote(ref, to, send_ref, recv_ref):
        return pltpu.make_async_remote_copy(
            src_ref=ref, dst_ref=ref, send_sem=send_ref, recv_sem=recv_ref, device_id=to, device_id_type=MESH
        )

    def whole(groups, part, phase, second, slot):
        dim = ORDERS[part][phase]
        ref = block(groups, part, phase, here[dim], both=not second)
        return remote(
            ref, device(dim, 1), send_sem.at[slot], recv_sem.at[stage(groups, part, phase, second)]
        )

    def send(groups, part, phase, second):
        slot = len(sent) % POOL
        if held[slot] is not None:
            held[slot].wait_send()
        dim = ORDERS[part][phase]
        for k, way in enumerate((1, -1)):
            if second:
                ref = block(groups, part, phase, (here[dim] - way + 4) % 4, half=k)
            else:
                ref = block(groups, part, phase, here[dim])
            remote(
                ref, device(dim, way), send_sem.at[slot], recv_sem.at[stage(groups, part, phase, second)]
            ).start()
        held[slot] = whole(groups, part, phase, second, slot)
        sent.append(slot)

    def arrive(groups, part, phase, second):
        whole(groups, part, phase, second, 0).wait_recv()

    kv_sent = []

    def start(copy):
        copy.start()
        kv_sent.append(copy)

    near, far = (cx + 3) % 4, (cx + 1) % 4
    other = (cx + 2) % 4
    keys, vals = pl.ds(0, 2), pl.ds(2, 2)
    kv_table = (
        ("y", kvl.at[cx, yl, keys]),
        ("x+", kvl.at[cx, yl, keys]),
        ("x-", kvl.at[cx, yl, keys]),
        ("x+", kvl.at[cx, 1 - yl, keys]),
        ("x-", kvl.at[cx, 1 - yl, keys]),
        ("x+", kvl.at[near, yl, keys]),
        ("x-", kvl.at[far, 1 - yl, keys]),
        ("x+", kvl.at[cx, yl, vals]),
        ("x-", kvl.at[cx, yl, vals]),
        ("y", kvl.at[cx, yl, vals]),
        ("x+", kvl.at[near, yl, 2]),
        ("x-", kvl.at[far, yl, 3]),
        ("y", kvl.at[near, yl, vals]),
        ("y", kvl.at[far, yl, vals]),
        ("y", kvl.at[other, yl, vals]),
    )

    def kv_hop(index):
        way, ref = kv_table[index]
        to = (cx * 2 + 1 - yl, core, dp) if way == "y" else device("x", 1 if way == "x+" else -1)
        return pltpu.make_async_remote_copy(
            src_ref=ref, dst_ref=ref, send_sem=kv_send.at[index], recv_sem=kv_recv.at[index],
            device_id=to, device_id_type=MESH,
        )

    kv_steps = {
        "K1": ((0,), ()),
        "K2": ((1, 2), ()),
        "K3": ((3, 4), (0,)),
        "K4": ((5,), (1,)),
        "K5": ((6,), (4,)),
        "V1": ((7, 8), ()),
        "V2": ((9,), ()),
        "V3": ((10, 11), (7, 8)),
        "V4": ((12, 13), (7, 8)),
        "V5": ((14,), (10, 11)),
    }
    kv_needs = {"own": (0, 9), "near": (1, 3, 7, 12), "far": (2, 4, 8, 13), "other": (5, 6, 10, 11, 14)}
    arrived = set()

    def kv_wait(indices):
        for index in indices:
            if index not in arrived:
                arrived.add(index)
                kv_hop(index).wait_recv()

    def rows_of(g, rows):
        return jnp.dot(x[rows, :], w[g].reshape(D, WIDTH), preferred_element_type=F32).astype(BF16)

    def project_kv(g, tile):
        @pl.when(core < 2)
        def _():
            rows = pl.ds(tile * TILE, TILE)
            result = rows_of(g, rows)
            (kb, vb)[g][rows, :] = result
            if tile == 1:
                for h in range(2):
                    kvl[cx, yl, 2 * g + h] = result[SEQ - TILE :, h * HD : (h + 1) * HD]

    def project_q(g):
        @pl.loop(0, ROWS // TILE)
        def _(i):
            rows = pl.ds(pl.multiple_of(i * TILE, 64), TILE)
            qb[g, rows, :] = rows_of(g + 2, rows)

    def short_bias():
        @pl.loop(0, 8)
        def _(i):
            first = pl.multiple_of(i * 128, 128)
            own_seg = seg_ref[:, pl.ds(first, 128)].astype(F32)
            query_seg = jnp.transpose(jnp.broadcast_to(own_seg, (128, 128)))
            window = jnp.maximum(i // 2 - 2, 0) * 256
            for j in range(6):
                start = pl.multiple_of(window + j * 128, 128)
                key_seg = jnp.broadcast_to(seg_ref[:, pl.ds(start, 128)].astype(F32), (128, 128))
                query_pos = first + lax.broadcasted_iota(jnp.int32, (128, 128), 0)
                key_pos = start + lax.broadcasted_iota(jnp.int32, (128, 128), 1)
                visible = (key_pos <= query_pos) & (key_seg == query_seg)
                bias_s[pl.ds(first, 128), pl.ds(j * 128, 128)] = jnp.where(visible, 0.0, HIDDEN)

    def long_bias():
        query_pos = yl * LONG + lax.broadcasted_iota(jnp.int32, (LONG, 2 * LONG), 0)
        key_pos = lax.broadcasted_iota(jnp.int32, (LONG, 2 * LONG), 1)
        visible = (key_pos <= query_pos) & (key_pos + cx * (2 * LONG) < len_ref[0])
        bias_l[...] = jnp.where(visible, 0.0, HIDDEN)

    def short_attention(g):
        kv = pl.ds((g // 2) * HD, HD)

        @pl.loop(0, 2)
        def _(h):
            head = pl.ds(pl.multiple_of(h * HD, HD), HD)

            def score(i):
                width = 256 * min(i + 1, 3)
                sc_s[i % 2, :, pl.ds(0, width)] = lax.dot_general(
                    qb[g, pl.ds(i * 256, 256), head],
                    kb[pl.ds(max(i - 2, 0) * 256, width), kv],
                    NT,
                    preferred_element_type=F32,
                )

            score(0)
            for i in range(4):
                if i < 3:
                    score(i + 1)
                width = 256 * min(i + 1, 3)
                rows = pl.ds(i * 256, 256)
                scores = sc_s[i % 2, :, pl.ds(0, width)] * SCALE + bias_s[rows, pl.ds(0, width)]
                top = jnp.max(scores, axis=1, keepdims=True)
                weights = jnp.exp2(scores - top)
                total = jnp.sum(weights, axis=1, keepdims=True)
                mixed = jnp.dot(
                    weights.astype(BF16),
                    vb[pl.ds(max(i - 2, 0) * 256, width), kv],
                    preferred_element_type=F32,
                )
                sob[g, rows, head] = (mixed / total).astype(BF16)

    def tiles(value):
        return [value[:, t * HD : (t + 1) * HD] for t in range(value.shape[1] // HD)]

    def fold(op, value):
        parts = tiles(value)
        while len(parts) > 1:
            parts = [
                op(parts[n], parts[n + 1]) if n + 1 < len(parts) else parts[n]
                for n in range(0, len(parts), 2)
            ]
        return parts[0]

    def pair(j, which):
        return jnp.concatenate([kvl[j, 0, which], kvl[j, 1, which]], axis=0)

    def long_parts(g, parts):
        kv = g // 2
        where = {"own": cx, "near": near, "far": far, "other": other}
        units = [(name, h) for name in parts for h in range(2)]

        def score(n):
            name, h = units[n]
            j = where[name]
            if name == "own":
                bias = bias_l[...]
            else:
                key_pos = j * (2 * LONG) + lax.broadcasted_iota(jnp.int32, (1, 2 * LONG), 1)
                bias = jnp.where((key_pos < len_ref[0]) & (j < cx), 0.0, HIDDEN)
            sc_l[n % 2] = bias + lax.dot_general(
                qb[g, pl.ds(SEQ, LONG), pl.ds(h * HD, HD)], pair(j, kv), NT, preferred_element_type=F32
            )

        score(0)
        for i, (name, h) in enumerate(units):
            if i + 1 < len(units):
                score(i + 1)
            n = 2 * g + h
            scores = sc_l[i % 2]
            largest = jnp.max(fold(jnp.maximum, scores), axis=1, keepdims=True) * SCALE
            top = jnp.broadcast_to(largest, (LONG, HD))
            if name != "own":
                top = jnp.maximum(mx[n], top)
            weights = jnp.exp2(scores * SCALE - jnp.concatenate([top] * 6, axis=1))
            mixed = jnp.dot(weights.astype(BF16), pair(where[name], 2 + kv), preferred_element_type=F32)
            if name == "own":
                tot[n] = fold(jnp.add, weights)
                acc[n] = mixed
            else:
                shrink = jnp.exp2(mx[n] - top)
                tot[n] = tot[n] * shrink + fold(jnp.add, weights)
                acc[n] = acc[n] * shrink + mixed
            mx[n] = top

    def long_finish(g):
        query_pos = blk * LONG + lax.broadcasted_iota(jnp.int32, (LONG, HD), 0)
        for h in range(2):
            mixed = acc[2 * g + h] / jnp.sum(tot[2 * g + h], axis=1, keepdims=True)
            mixed = jnp.where(query_pos < len_ref[0], mixed, 0.0)
            lob[g, :, pl.ds(h * HD, HD)] = mixed.astype(BF16)

    outs = []
    peer_outs = []

    def ship_short(g):
        columns = pl.ds(pl.multiple_of(core * SEQ + g * WIDTH, WIDTH), WIDTH)
        theirs = pl.ds(pl.multiple_of((1 - core) * HALF, HALF), HALF)
        peer = pltpu.make_async_remote_copy(
            src_ref=sob.at[g, theirs], dst_ref=so_hbm.at[0, :, columns],
            send_sem=out_send.at[g], recv_sem=out_recv.at[g], device_id=sibling, device_id_type=MESH,
        )
        mine = pltpu.make_async_copy(sob.at[g, my_rows], so_hbm.at[0, :, columns], out_own.at[g])
        peer.start()
        mine.start()
        peer_outs.append(peer)
        outs.append(mine)

    def ship_long(g):
        mine = pltpu.make_async_copy(
            lob.at[g], lo_hbm.at[0, :, pl.ds(g * WIDTH, WIDTH)], out_own.at[4 + g]
        )
        mine.start()
        outs.append(mine)

    groups_of = {g: groups for groups in FIRST for g in groups}
    parts_of = [[p for p in range(3) if PARTS[g][p][1]] for g in range(GROUPS)]

    def step(name):
        kind, rest = name[:2], name[2:]
        if kind[0] == "P":
            phase, second, g, part = int(kind[1]), rest[0] == "b", int(rest[1]), int(rest[2])
            groups = groups_of[g] if phase == 0 else (g,)
            if second:
                arrive(groups, part, phase, False)
            elif phase == 1:
                arrive_first(g, part)
            elif phase == 2:
                arrive(groups, part, 1, True)
            send(groups, part, phase, second)
        elif kind[0] in "KV":
            sends, needs = kv_steps[name]
            kv_wait(needs)
            for index in sends:
                start(kv_hop(index))
        elif kind[0] == "W":
            g = int(kind[1])
            for part in parts_of[g]:
                arrive((g,), part, 2, True)
        elif kind == "pr":
            if len(rest) == 2:
                project_kv(int(rest[0]), int(rest[1]))
            else:
                project_q(int(rest) - 2)
        elif kind == "sh":
            short_attention(int(rest))
            ship_short(int(rest))
        elif kind == "lo":
            g = int(rest[0])
            names = {"o": "own", "n": "near", "f": "far", "t": "other"}
            parts = [names[letter] for letter in rest[1:]]
            for part in parts:
                kv_wait(kv_needs[part])
            long_parts(g, parts)
            if parts[-1] == "other":
                long_finish(g)
                ship_long(g)
        elif name == "X":
            own_x.wait()
            own_l.wait()
            peer_x.wait_recv()
        else:
            peer_x.start()
            long_bias()
            short_bias()

    met = set()

    def arrive_first(g, part):
        groups = groups_of[g]
        if (groups, part) not in met:
            met.add((groups, part))
            arrive(groups, part, 0, True)

    for name in ORDER:
        step(name)

    peer_x.wait_send()
    for copy in kv_sent + [copy for copy in held if copy is not None]:
        copy.wait_send()
    for copy in outs:
        copy.wait()
    for copy in peer_outs:
        copy.wait()


def place(short_in, long_in, short_out, long_out, short_buf, long_buf, in_sem, out_sem):
    pieces = [
        (short_in.at[0, pl.ds(n * HALF // 4, HALF // 4)], short_buf.at[n], short_out.at[0, pl.ds(n * HALF // 4, HALF // 4)])
        for n in range(4)
    ] + [
        (long_in.at[0, pl.ds(n * LONG // 2, LONG // 2)], long_buf.at[n], long_out.at[0, pl.ds(n * LONG // 2, LONG // 2)])
        for n in range(2)
    ]
    fetches = [pltpu.make_async_copy(src, buf, in_sem.at[n]) for n, (src, buf, _) in enumerate(pieces)]
    stores = [pltpu.make_async_copy(buf, dst, out_sem.at[n]) for n, (_, buf, dst) in enumerate(pieces)]
    for copy in fetches:
        copy.start()
    for fetch, store in zip(fetches, stores):
        fetch.wait()
        store.start()
    for copy in stores:
        copy.wait()


def local(short_tokens, short_segments, long_tokens, long_lengths, w_query, w_key, w_value):
    anywhere = pl.BlockSpec(memory_space=pl.ANY)
    vmem = pl.BlockSpec(memory_space=pltpu.VMEM)
    smem = pl.BlockSpec(memory_space=pltpu.SMEM)
    dma = pltpu.SemaphoreType.DMA
    shorts, longs = pl.pallas_call(
        kernel,
        out_shape=(
            jax.ShapeDtypeStruct((1, HALF, 2 * SEQ), BF16),
            jax.ShapeDtypeStruct((1, LONG, SEQ), BF16),
        ),
        in_specs=[anywhere, vmem, anywhere, smem, anywhere, anywhere, anywhere],
        out_specs=(anywhere, anywhere),
        scratch_shapes=[
            pltpu.VMEM((GROUPS, 4, 2, 4, 2, 64, WIDTH), BF16),
            pltpu.VMEM((ROWS, D), BF16),
            pltpu.VMEM((ROWS, WIDTH), BF16),
            pltpu.VMEM((ROWS, WIDTH), BF16),
            pltpu.VMEM((4, ROWS, WIDTH), BF16),
            pltpu.VMEM((4, 2, 4, LONG, HD), BF16),
            pltpu.VMEM((4, SEQ, WIDTH), BF16),
            pltpu.VMEM((4, LONG, WIDTH), BF16),
            pltpu.VMEM((SEQ, 768), F32),
            pltpu.VMEM((LONG, 2 * LONG), F32),
            pltpu.VMEM((2, 256, 768), F32),
            pltpu.VMEM((2, LONG, 2 * LONG), F32),
            pltpu.VMEM((8, LONG, HD), F32),
            pltpu.VMEM((8, LONG, HD), F32),
            pltpu.VMEM((8, LONG, HD), F32),
            dma((POOL,)),
            dma((6 * (2 * GROUPS + len(FIRST)),)),
            dma((15,)),
            dma((15,)),
            dma((4,)),
            dma((6,)),
            dma((4,)),
            dma((4,)),
            dma((8,)),
        ],
        compiler_params=pltpu.CompilerParams(
            collective_id=0, has_side_effects=True, vmem_limit_bytes=VMEM
        ),
    )(short_tokens, short_segments, long_tokens, long_lengths, w_query, w_key, w_value)
    return pl.pallas_call(
        place,
        out_shape=(
            jax.ShapeDtypeStruct(shorts.shape, BF16),
            jax.ShapeDtypeStruct(longs.shape, BF16),
        ),
        in_specs=[anywhere, anywhere],
        out_specs=(anywhere, anywhere),
        scratch_shapes=[
            pltpu.VMEM((4, HALF // 4, 2 * SEQ), BF16),
            pltpu.VMEM((2, LONG // 2, SEQ), BF16),
            dma((6,)),
            dma((6,)),
        ],
    )(shorts, longs)


def solution(mesh):
    return jax.shard_map(
        local,
        mesh=mesh,
        in_specs=(
            P(("blk", "dp"), "uly", None),
            P(("blk", "dp"), None),
            P("dp", "blk", None),
            P("dp"),
            P(("blk", "dp"), "uly"),
            P(("blk", "dp"), "uly"),
            P(("blk", "dp"), "uly"),
        ),
        out_specs=(P(("blk", "dp"), "uly", None), P("dp", "blk", "uly")),
        check_vma=False,
    )
```

```python
import math

import jax
import jax.numpy as jnp
from jax import lax
from jax.experimental import pallas as pl
from jax.experimental.pallas import tpu as pltpu
from jax.sharding import PartitionSpec as P

MESH = pl.DeviceIdType.MESH
BF16 = jnp.bfloat16
F32 = jnp.float32
HD = 128
D = 4096
SEQ = 1024
HALF = 512
LONG = 384
ROWS = SEQ + LONG
TILE = ROWS // 2
GROUPS = 6
WIDTH = 256
HIDDEN = -1e30
POOL = 40
VMEM = 60_000_000
SCALE = math.log2(math.e) / math.sqrt(HD)

ORDERS = ("xyz", "yzx", "zxy")
PARTS = (
    ((0, 32), (32, 16), (48, 16)),
    ((0, 16), (16, 16), (32, 32)),
    ((0, 32), (32, 16), (48, 16)),
    ((0, 32), (32, 16), (48, 16)),
    ((0, 16), (16, 32), (48, 16)),
    ((0, 16), (16, 32), (48, 16)),
)
FIRST = ((0,), (1,), (2, 3), (4, 5),)
ORDER = (
    "P0a01", "P0a02", "P0a00", "P0a20", "P0a21", "P0a12", "P0a11", "P0a42", "P0a10", "P0a40", "B", "P0a41", "P0a22",
    "P0b02", "P0b01", "P0b00", "P0b12", "P0b21", "P0b11", "P0b42", "P0b20", "P0b10", "P0b22", "P0b41", "P0b40",
    "P1a02", "P1a01", "P1a00", "P1a12", "P1a21", "P1a31", "P1a11", "P1a52", "P1a42", "P1a22", "P1a30", "P1a32",
    "P1a10", "P1a41", "P1a40", "P1b02", "P1b01", "P1b21", "P1b00", "P1b12", "P1b31", "P1a51", "P1b11", "P1b52",
    "P1a50", "P1b30", "P1b42", "P1b10", "P1b41", "P1b22", "P1b40", "P2a01", "P2a21", "P1b32", "P1a20", "P2a00",
    "P2a31", "P2a02", "P1b50", "P2a12", "P2a10", "P2a11", "P2a41", "P2a42", "P2a40", "P2b01", "P1b20", "P2b02",
    "P2b21", "P2a32", "P2b00", "P2b31", "P2b10", "P2b12", "P2a30", "P2b11", "P2b40", "P2b42", "P2a22", "P2a20",
    "P2b41", "P2b32", "W0", "X", "pr01", "K2", "K1", "pr00", "P2b30", "W1", "pr11", "V1", "V2", "pr10", "P2b22",
    "W4", "pr4", "P2b20", "sh2", "P1b51", "K3", "W3", "pr3", "V4", "V3", "P2a50", "sh1", "W2", "P2a51", "lo1o",
    "K5", "lo2o", "pr2", "P2b50", "V5", "sh0", "K4", "lo0o", "P2b51", "P2a52", "lo0nf", "lo2nf", "lo0t", "P2b52",
    "lo2t", "lo1nft", "W5", "pr5", "sh3", "lo3onft",
)

NT = (((1,), (1,)), ((), ()))


def kernel(
    xs_hbm, seg_ref, xl_hbm, len_ref, wq_hbm, wk_hbm, wv_hbm,
    so_hbm, lo_hbm,
    w, x, kb, vb, qb, kvl, sob, lob, bias_s, bias_l, sc_s, sc_l, acc, mx, tot,
    send_sem, recv_sem, kv_send, kv_recv, x_sem, own_sem, out_send, out_recv, out_own,
):
    blk, core, dp = lax.axis_index("blk"), lax.axis_index("uly"), lax.axis_index("dp")
    cx, yl = blk // 2, blk % 2
    cz, yh = dp // 2, dp % 2
    cy = yh * 2 + yl
    here = {"x": cx, "y": cy, "z": cz}

    def device(dim, step):
        at = dict(here)
        at[dim] = (here[dim] + step + 4) % 4
        return (at["x"] * 2 + at["y"] % 2, core, at["z"] * 2 + at["y"] // 2)

    sibling = (blk, 1 - core, dp)

    own = [
        pltpu.make_async_copy(wk_hbm, w.at[0, cx, yl, cz, yh], own_sem.at[0]),
        pltpu.make_async_copy(wv_hbm, w.at[1, cx, yl, cz, yh], own_sem.at[1]),
    ]
    for g in range(4):
        own.append(
            pltpu.make_async_copy(
                wq_hbm.at[:, pl.ds(g * WIDTH, WIDTH)], w.at[2 + g, cx, yl, cz, yh], own_sem.at[2 + g]
            )
        )
    my_rows = pl.ds(pl.multiple_of(core * HALF, HALF), HALF)
    own_x = pltpu.make_async_copy(xs_hbm.at[0], x.at[my_rows], x_sem.at[0])
    own_l = pltpu.make_async_copy(xl_hbm.at[0], x.at[pl.ds(SEQ, LONG)], x_sem.at[1])
    for copy in own + [own_l, own_x]:
        copy.start()

    barrier = pltpu.get_barrier_semaphore()
    for dim in "xyz":
        for step in (1, -1):
            pl.semaphore_signal(barrier, inc=1, device_id=device(dim, step), device_id_type=MESH)
    pl.semaphore_signal(barrier, inc=1, device_id=sibling, device_id_type=MESH)
    pl.semaphore_wait(barrier, 7)

    peer_x = pltpu.make_async_remote_copy(
        src_ref=xs_hbm.at[0], dst_ref=x.at[my_rows], send_sem=x_sem.at[2], recv_sem=x_sem.at[3],
        device_id=sibling, device_id_type=MESH,
    )
    for copy in own:
        copy.wait()

    def block(groups, part, phase, position, half=None, both=False):
        first, count = PARTS[groups[0]][part]
        order = ORDERS[part]
        dim = order[phase]
        at = dict(here)
        at[dim] = position
        done = order[:phase]
        ix = slice(None) if "x" in done else at["x"]
        iz = slice(None) if "z" in done else at["z"]
        il = slice(None) if "y" in done else at["y"] % 2
        ih = slice(None) if "y" in done else at["y"] // 2
        columns = slice(None)
        if both:
            two = pl.ds(0, 2)
            ix, il, iz = two if dim == "x" else ix, two if dim == "y" else il, two if dim == "z" else iz
        if half is not None:
            if phase == 0:
                columns = pl.ds(half * 128, 128)
            elif order[0] == "x":
                ix = pl.ds(2 * half, 2)
            elif order[0] == "z":
                iz = pl.ds(2 * half, 2)
            else:
                il = half
        which = pl.ds(groups[0], len(groups)) if len(groups) > 1 else groups[0]
        return w.at[which, ix, il, iz, ih, pl.ds(first, count), columns]

    stage_of = {}
    sent = []
    held = [None] * POOL

    def stage(groups, part, phase, second):
        return stage_of.setdefault((groups, part, phase, second), len(stage_of))

    def remote(ref, to, send_ref, recv_ref):
        return pltpu.make_async_remote_copy(
            src_ref=ref, dst_ref=ref, send_sem=send_ref, recv_sem=recv_ref, device_id=to, device_id_type=MESH
        )

    def whole(groups, part, phase, second, slot):
        dim = ORDERS[part][phase]
        ref = block(groups, part, phase, here[dim], both=not second)
        return remote(
            ref, device(dim, 1), send_sem.at[slot], recv_sem.at[stage(groups, part, phase, second)]
        )

    def send(groups, part, phase, second):
        slot = len(sent) % POOL
        if held[slot] is not None:
            held[slot].wait_send()
        dim = ORDERS[part][phase]
        for k, way in enumerate((1, -1)):
            if second:
                ref = block(groups, part, phase, (here[dim] - way + 4) % 4, half=k)
            else:
                ref = block(groups, part, phase, here[dim])
            remote(
                ref, device(dim, way), send_sem.at[slot], recv_sem.at[stage(groups, part, phase, second)]
            ).start()
        held[slot] = whole(groups, part, phase, second, slot)
        sent.append(slot)

    def arrive(groups, part, phase, second):
        whole(groups, part, phase, second, 0).wait_recv()

    kv_sent = []

    def start(copy):
        copy.start()
        kv_sent.append(copy)

    near, far = (cx + 3) % 4, (cx + 1) % 4
    other = (cx + 2) % 4
    keys, vals = pl.ds(0, 2), pl.ds(2, 2)
    kv_table = (
        ("y", kvl.at[cx, yl, keys]),
        ("x+", kvl.at[cx, yl, keys]),
        ("x-", kvl.at[cx, yl, keys]),
        ("x+", kvl.at[cx, 1 - yl, keys]),
        ("x-", kvl.at[cx, 1 - yl, keys]),
        ("x+", kvl.at[near, yl, keys]),
        ("x-", kvl.at[far, 1 - yl, keys]),
        ("x+", kvl.at[cx, yl, vals]),
        ("x-", kvl.at[cx, yl, vals]),
        ("y", kvl.at[cx, yl, vals]),
        ("x+", kvl.at[near, yl, 2]),
        ("x-", kvl.at[far, yl, 3]),
        ("y", kvl.at[near, yl, vals]),
        ("y", kvl.at[far, yl, vals]),
        ("y", kvl.at[other, yl, vals]),
    )

    def kv_hop(index):
        way, ref = kv_table[index]
        to = (cx * 2 + 1 - yl, core, dp) if way == "y" else device("x", 1 if way == "x+" else -1)
        return pltpu.make_async_remote_copy(
            src_ref=ref, dst_ref=ref, send_sem=kv_send.at[index], recv_sem=kv_recv.at[index],
            device_id=to, device_id_type=MESH,
        )

    kv_steps = {
        "K1": ((0,), ()),
        "K2": ((1, 2), ()),
        "K3": ((3, 4), (0,)),
        "K4": ((5,), (1,)),
        "K5": ((6,), (4,)),
        "V1": ((7, 8), ()),
        "V2": ((9,), ()),
        "V3": ((10, 11), (7, 8)),
        "V4": ((12, 13), (7, 8)),
        "V5": ((14,), (10, 11)),
    }
    kv_needs = {"own": (0, 9), "near": (1, 3, 7, 12), "far": (2, 4, 8, 13), "other": (5, 6, 10, 11, 14)}
    arrived = set()

    def kv_wait(indices):
        for index in indices:
            if index not in arrived:
                arrived.add(index)
                kv_hop(index).wait_recv()

    def rows_of(g, rows):
        return jnp.dot(x[rows, :], w[g].reshape(D, WIDTH), preferred_element_type=F32).astype(BF16)

    def project_kv(g, tile):
        @pl.when(core < 2)
        def _():
            rows = pl.ds(tile * TILE, TILE)
            result = rows_of(g, rows)
            (kb, vb)[g][rows, :] = result
            if tile == 1:
                for h in range(2):
                    kvl[cx, yl, 2 * g + h] = result[SEQ - TILE :, h * HD : (h + 1) * HD]

    def project_q(g):
        @pl.loop(0, ROWS // TILE)
        def _(i):
            rows = pl.ds(pl.multiple_of(i * TILE, 64), TILE)
            qb[g, rows, :] = rows_of(g + 2, rows)

    def short_bias():
        @pl.loop(0, 8)
        def _(i):
            first = pl.multiple_of(i * 128, 128)
            own_seg = seg_ref[:, pl.ds(first, 128)].astype(F32)
            query_seg = jnp.transpose(jnp.broadcast_to(own_seg, (128, 128)))
            window = jnp.maximum(i // 2 - 2, 0) * 256
            for j in range(6):
                start = pl.multiple_of(window + j * 128, 128)
                key_seg = jnp.broadcast_to(seg_ref[:, pl.ds(start, 128)].astype(F32), (128, 128))
                query_pos = first + lax.broadcasted_iota(jnp.int32, (128, 128), 0)
                key_pos = start + lax.broadcasted_iota(jnp.int32, (128, 128), 1)
                visible = (key_pos <= query_pos) & (key_seg == query_seg)
                bias_s[pl.ds(first, 128), pl.ds(j * 128, 128)] = jnp.where(visible, 0.0, HIDDEN)

    def long_bias():
        query_pos = yl * LONG + lax.broadcasted_iota(jnp.int32, (LONG, 2 * LONG), 0)
        key_pos = lax.broadcasted_iota(jnp.int32, (LONG, 2 * LONG), 1)
        visible = (key_pos <= query_pos) & (key_pos + cx * (2 * LONG) < len_ref[0])
        bias_l[...] = jnp.where(visible, 0.0, HIDDEN)

    def short_attention(g):
        kv = pl.ds((g // 2) * HD, HD)
        items = [(i, h) for i in range(4) for h in range(2)]

        def score(n):
            i, h = items[n]
            width = 256 * min(i + 1, 3)
            sc_s[n % 2, :, pl.ds(0, width)] = lax.dot_general(
                qb[g, pl.ds(i * 256, 256), pl.ds(h * HD, HD)],
                kb[pl.ds(max(i - 2, 0) * 256, width), kv],
                NT,
                preferred_element_type=F32,
            )

        score(0)
        for n, (i, h) in enumerate(items):
            if n + 1 < len(items):
                score(n + 1)
            width = 256 * min(i + 1, 3)
            rows = pl.ds(i * 256, 256)
            scores = sc_s[n % 2, :, pl.ds(0, width)] * SCALE + bias_s[rows, pl.ds(0, width)]
            top = jnp.max(scores, axis=1, keepdims=True)
            weights = jnp.exp2(scores - top)
            total = jnp.sum(weights, axis=1, keepdims=True)
            mixed = jnp.dot(
                weights.astype(BF16),
                vb[pl.ds(max(i - 2, 0) * 256, width), kv],
                preferred_element_type=F32,
            )
            sob[g, rows, pl.ds(h * HD, HD)] = (mixed / total).astype(BF16)

    def tiles(value):
        return [value[:, t * HD : (t + 1) * HD] for t in range(value.shape[1] // HD)]

    def fold(op, value):
        parts = tiles(value)
        while len(parts) > 1:
            parts = [
                op(parts[n], parts[n + 1]) if n + 1 < len(parts) else parts[n]
                for n in range(0, len(parts), 2)
            ]
        return parts[0]

    def pair(j, which):
        return jnp.concatenate([kvl[j, 0, which], kvl[j, 1, which]], axis=0)

    def long_parts(g, parts):
        kv = g // 2
        where = {"own": cx, "near": near, "far": far, "other": other}
        units = [(name, h) for name in parts for h in range(2)]

        def score(n):
            name, h = units[n]
            j = where[name]
            if name == "own":
                bias = bias_l[...]
            else:
                key_pos = j * (2 * LONG) + lax.broadcasted_iota(jnp.int32, (1, 2 * LONG), 1)
                bias = jnp.where((key_pos < len_ref[0]) & (j < cx), 0.0, HIDDEN)
            sc_l[n % 2] = bias + lax.dot_general(
                qb[g, pl.ds(SEQ, LONG), pl.ds(h * HD, HD)], pair(j, kv), NT, preferred_element_type=F32
            )

        score(0)
        for i, (name, h) in enumerate(units):
            if i + 1 < len(units):
                score(i + 1)
            n = 2 * g + h
            scores = sc_l[i % 2]
            largest = jnp.max(fold(jnp.maximum, scores), axis=1, keepdims=True) * SCALE
            top = jnp.broadcast_to(largest, (LONG, HD))
            if name != "own":
                top = jnp.maximum(mx[n], top)
            weights = jnp.exp2(scores * SCALE - jnp.concatenate([top] * 6, axis=1))
            mixed = jnp.dot(weights.astype(BF16), pair(where[name], 2 + kv), preferred_element_type=F32)
            if name == "own":
                tot[n] = fold(jnp.add, weights)
                acc[n] = mixed
            else:
                shrink = jnp.exp2(mx[n] - top)
                tot[n] = tot[n] * shrink + fold(jnp.add, weights)
                acc[n] = acc[n] * shrink + mixed
            mx[n] = top

    def long_finish(g):
        query_pos = blk * LONG + lax.broadcasted_iota(jnp.int32, (LONG, HD), 0)
        for h in range(2):
            mixed = acc[2 * g + h] / jnp.sum(tot[2 * g + h], axis=1, keepdims=True)
            mixed = jnp.where(query_pos < len_ref[0], mixed, 0.0)
            lob[g, :, pl.ds(h * HD, HD)] = mixed.astype(BF16)

    outs = []
    peer_outs = []

    def ship_short(g):
        columns = pl.ds(pl.multiple_of(core * SEQ + g * WIDTH, WIDTH), WIDTH)
        theirs = pl.ds(pl.multiple_of((1 - core) * HALF, HALF), HALF)
        peer = pltpu.make_async_remote_copy(
            src_ref=sob.at[g, theirs], dst_ref=so_hbm.at[0, :, columns],
            send_sem=out_send.at[g], recv_sem=out_recv.at[g], device_id=sibling, device_id_type=MESH,
        )
        mine = pltpu.make_async_copy(sob.at[g, my_rows], so_hbm.at[0, :, columns], out_own.at[g])
        peer.start()
        mine.start()
        peer_outs.append(peer)
        outs.append(mine)

    def ship_long(g):
        mine = pltpu.make_async_copy(
            lob.at[g], lo_hbm.at[0, :, pl.ds(g * WIDTH, WIDTH)], out_own.at[4 + g]
        )
        mine.start()
        outs.append(mine)

    groups_of = {g: groups for groups in FIRST for g in groups}
    parts_of = [[p for p in range(3) if PARTS[g][p][1]] for g in range(GROUPS)]

    def step(name):
        kind, rest = name[:2], name[2:]
        if kind[0] == "P":
            phase, second, g, part = int(kind[1]), rest[0] == "b", int(rest[1]), int(rest[2])
            groups = groups_of[g] if phase == 0 else (g,)
            if second:
                arrive(groups, part, phase, False)
            elif phase == 1:
                arrive_first(g, part)
            elif phase == 2:
                arrive(groups, part, 1, True)
            send(groups, part, phase, second)
        elif kind[0] in "KV":
            sends, needs = kv_steps[name]
            kv_wait(needs)
            for index in sends:
                start(kv_hop(index))
        elif kind[0] == "W":
            g = int(kind[1])
            for part in parts_of[g]:
                arrive((g,), part, 2, True)
        elif kind == "pr":
            if len(rest) == 2:
                project_kv(int(rest[0]), int(rest[1]))
            else:
                project_q(int(rest) - 2)
        elif kind == "sh":
            short_attention(int(rest))
            ship_short(int(rest))
        elif kind == "lo":
            g = int(rest[0])
            names = {"o": "own", "n": "near", "f": "far", "t": "other"}
            parts = [names[letter] for letter in rest[1:]]
            for part in parts:
                kv_wait(kv_needs[part])
            long_parts(g, parts)
            if parts[-1] == "other":
                long_finish(g)
                ship_long(g)
        elif name == "X":
            own_x.wait()
            own_l.wait()
            peer_x.wait_recv()
        else:
            peer_x.start()
            long_bias()
            short_bias()

    met = set()

    def arrive_first(g, part):
        groups = groups_of[g]
        if (groups, part) not in met:
            met.add((groups, part))
            arrive(groups, part, 0, True)

    for name in ORDER:
        step(name)

    peer_x.wait_send()
    for copy in kv_sent + [copy for copy in held if copy is not None]:
        copy.wait_send()
    for copy in outs:
        copy.wait()
    for copy in peer_outs:
        copy.wait()


def place(short_in, long_in, short_out, long_out, short_buf, long_buf, in_sem, out_sem):
    pieces = [
        (short_in.at[0, pl.ds(n * HALF // 4, HALF // 4)], short_buf.at[n], short_out.at[0, pl.ds(n * HALF // 4, HALF // 4)])
        for n in range(4)
    ] + [
        (long_in.at[0, pl.ds(n * LONG // 2, LONG // 2)], long_buf.at[n], long_out.at[0, pl.ds(n * LONG // 2, LONG // 2)])
        for n in range(2)
    ]
    fetches = [pltpu.make_async_copy(src, buf, in_sem.at[n]) for n, (src, buf, _) in enumerate(pieces)]
    stores = [pltpu.make_async_copy(buf, dst, out_sem.at[n]) for n, (_, buf, dst) in enumerate(pieces)]
    for copy in fetches:
        copy.start()
    for fetch, store in zip(fetches, stores):
        fetch.wait()
        store.start()
    for copy in stores:
        copy.wait()


def local(short_tokens, short_segments, long_tokens, long_lengths, w_query, w_key, w_value):
    anywhere = pl.BlockSpec(memory_space=pl.ANY)
    vmem = pl.BlockSpec(memory_space=pltpu.VMEM)
    smem = pl.BlockSpec(memory_space=pltpu.SMEM)
    dma = pltpu.SemaphoreType.DMA
    shorts, longs = pl.pallas_call(
        kernel,
        out_shape=(
            jax.ShapeDtypeStruct((1, HALF, 2 * SEQ), BF16),
            jax.ShapeDtypeStruct((1, LONG, SEQ), BF16),
        ),
        in_specs=[anywhere, vmem, anywhere, smem, anywhere, anywhere, anywhere],
        out_specs=(anywhere, anywhere),
        scratch_shapes=[
            pltpu.VMEM((GROUPS, 4, 2, 4, 2, 64, WIDTH), BF16),
            pltpu.VMEM((ROWS, D), BF16),
            pltpu.VMEM((ROWS, WIDTH), BF16),
            pltpu.VMEM((ROWS, WIDTH), BF16),
            pltpu.VMEM((4, ROWS, WIDTH), BF16),
            pltpu.VMEM((4, 2, 4, LONG, HD), BF16),
            pltpu.VMEM((4, SEQ, WIDTH), BF16),
            pltpu.VMEM((4, LONG, WIDTH), BF16),
            pltpu.VMEM((SEQ, 768), F32),
            pltpu.VMEM((LONG, 2 * LONG), F32),
            pltpu.VMEM((2, 256, 768), F32),
            pltpu.VMEM((2, LONG, 2 * LONG), F32),
            pltpu.VMEM((8, LONG, HD), F32),
            pltpu.VMEM((8, LONG, HD), F32),
            pltpu.VMEM((8, LONG, HD), F32),
            dma((POOL,)),
            dma((6 * (2 * GROUPS + len(FIRST)),)),
            dma((15,)),
            dma((15,)),
            dma((4,)),
            dma((6,)),
            dma((4,)),
            dma((4,)),
            dma((8,)),
        ],
        compiler_params=pltpu.CompilerParams(
            collective_id=0, has_side_effects=True, vmem_limit_bytes=VMEM
        ),
    )(short_tokens, short_segments, long_tokens, long_lengths, w_query, w_key, w_value)
    return pl.pallas_call(
        place,
        out_shape=(
            jax.ShapeDtypeStruct(shorts.shape, BF16),
            jax.ShapeDtypeStruct(longs.shape, BF16),
        ),
        in_specs=[anywhere, anywhere],
        out_specs=(anywhere, anywhere),
        scratch_shapes=[
            pltpu.VMEM((4, HALF // 4, 2 * SEQ), BF16),
            pltpu.VMEM((2, LONG // 2, SEQ), BF16),
            dma((6,)),
            dma((6,)),
        ],
    )(shorts, longs)


def solution(mesh):
    return jax.shard_map(
        local,
        mesh=mesh,
        in_specs=(
            P(("blk", "dp"), "uly", None),
            P(("blk", "dp"), None),
            P("dp", "blk", None),
            P("dp"),
            P(("blk", "dp"), "uly"),
            P(("blk", "dp"), "uly"),
            P(("blk", "dp"), "uly"),
        ),
        out_specs=(P(("blk", "dp"), "uly", None), P("dp", "blk", "uly")),
        check_vma=False,
    )
```
